128 devices in a mesh: row: 16 (over x, z), col: 8 (over y, core).
Axes of the slice: x: 4, y: 4, z: 4, core: 2. Of those that a mesh axis runs over, the one named last changes fastest.
Arguments:
- old_params: float32 [2, 256, 32768], P(None, ('row', 'col')), may hold values from -0.12 to 0.12
- old_first: float32 [2, 256, 32768], P(None, ('row', 'col')), may hold values from -1.8 to 1.8
- old_second: float32 [2, 256, 32768], P(None, ('row', 'col')), may hold values from 0.001 to 1
- gradients: float32 [2, 128, 65536], P(None, ('row', 'col')), may hold values from -250 to 250
- old_table: int32 [2, 256], replicated, may hold values from 0 to 255, as said below
- new_table: int32 [2, 128], replicated, may hold values from 0 to 127, as said below
Outputs:
- new_params: float32 [2, 128, 65536], P(None, ('row', 'col'))
- new_first: float32 [2, 128, 65536], P(None, ('row', 'col'))
- new_second: float32 [2, 128, 65536], P(None, ('row', 'col'))
The draws below stay inside these ranges and needn't reach their ends.
Inputs may be any that keep to these rules, and one draw needn't show every extreme that they name: old_table[t, p] = p XOR k for one k per tensor. new_table[t, q] = q XOR k for one k per tensor.
All inputs are finite; a program needn't handle non-finite values.
Results may differ from the reference program's by a relative error of at most 0.00002.
Values sent between devices are 32-bit elements; how exact they have to be, the bound alone decides.
A program may use at most 64 MiB of HBM per device.

```python
import math
import jax
import jax.numpy as jnp

STEP = 100
NT = 2
ELEMS = 8388608
OLD_SHARDS = 256
OB = 32768
DEVICES = 128


def draw_old_table(key, part):
    folded = jax.random.fold_in(key, 11)
    offsets = jax.random.randint(folded, (NT, 1), 0, OLD_SHARDS)
    return jnp.bitwise_xor(jnp.arange(OLD_SHARDS, dtype=jnp.int32)[None, :], offsets).astype(jnp.int32)


def draw_new_table(key, part):
    folded = jax.random.fold_in(key, 23)
    offsets = jax.random.randint(folded, (NT, 1), 0, DEVICES)
    return jnp.bitwise_xor(jnp.arange(DEVICES, dtype=jnp.int32)[None, :], offsets).astype(jnp.int32)


def draw_gradients(key, part):
    folded = jax.random.fold_in(key, 37)
    key_private = jax.random.fold_in(folded, 0)
    position = jnp.arange(DEVICES, dtype=jnp.float32)[None, :, None]
    rising = 1.0 + 2.0 * position / max(DEVICES - 1, 1)
    private = jnp.clip(jax.random.normal(key_private, (NT, DEVICES, 2 * OB)), -8.0, 8.0)
    return (rising * private).astype(jnp.float32)


def shard_levels(own_key, shape, cuts, smallest, top_value):
    factor_of, own = 1.0, jax.random.fold_in(own_key, 6)
    for axis_at, parts in cuts:
        draws = jnp.exp(jax.random.uniform(jax.random.fold_in(own, axis_at), (parts,), jnp.float32, smallest / len(cuts), top_value / len(cuts)))
        factor_of = factor_of * jnp.repeat(draws, shape[axis_at] // parts).reshape([-1 if axis == axis_at else 1 for axis in range(len(shape))])
    return factor_of


def noise(key, shape, spread, most, cuts=(), held_as=jnp.bfloat16):
    gain = shard_levels(key, shape, cuts, -0.22, 0.18) if cuts else 1.0
    entries = jax.random.normal(key, shape, jnp.float32) * spread * gain
    return jnp.minimum(jnp.maximum(entries, -most), most).astype(held_as)


def setup_inputs(seed: int = 0) -> dict:
    seeds = jax.random.split(jax.random.key(seed), 7)
    return {
        "old_params": noise(seeds[0], (NT, OLD_SHARDS, OB), 0.02, 0.12, ((1, 128),), jnp.float32),
        "old_first": noise(seeds[1], (NT, OLD_SHARDS, OB), 0.3, 1.8, ((1, 128),), jnp.float32),
        "old_second": jnp.clip(jnp.exp(math.log(1.0) - 6.9077552 * jax.random.uniform(seeds[2], (NT, OLD_SHARDS, OB), jnp.float32) ** shard_levels(seeds[2], (NT, OLD_SHARDS, OB), ((1, 128),), -0.2, 0.2)), 0.001, 1.0),
        "gradients": draw_gradients(jax.random.fold_in(seeds[6], 71), 0),
        "old_table": draw_old_table(jax.random.fold_in(seeds[6], 71), 0),
        "new_table": draw_new_table(jax.random.fold_in(seeds[6], 71), 0),
    }


beta_one = 0.9
beta_two = 0.95
epsilon = 1e-08
learn_rate = 0.001
decay_rate = 0.1

def relayout(old_state, old_table, new_table):
    tensors = jnp.arange(old_state.shape[0], dtype=jnp.int32)[:, None]
    blocks = jnp.zeros_like(old_state).at[tensors, old_table].set(old_state)
    paired = blocks.reshape(old_state.shape[0], old_state.shape[1] // 2, 2 * old_state.shape[2])
    return paired[tensors, new_table]

def adam_update(params, first_moment, second_moment, gradients, clip_factor):
    scaled = clip_factor * gradients
    first_new = beta_one * first_moment + (1.0 - beta_one) * scaled
    second_new = beta_two * second_moment + (1.0 - beta_two) * scaled * scaled
    bias_first = 1.0 - beta_one ** STEP
    bias_second = 1.0 - beta_two ** STEP
    update = first_new / bias_first / (jnp.sqrt(second_new / bias_second) + epsilon)
    params_new = params - learn_rate * (update + decay_rate * params)
    return (params_new, first_new, second_new)

def reference(old_params, old_first, old_second, gradients, old_table, new_table):
    moved_params = relayout(old_params, old_table, new_table)
    moved_first = relayout(old_first, old_table, new_table)
    moved_second = relayout(old_second, old_table, new_table)
    grad_norm = jnp.sqrt(jnp.sum(gradients * gradients))
    limit = jnp.float32(0.5 * (NT * ELEMS) ** 0.5)
    clip_factor = limit / jnp.maximum(grad_norm, limit)
    return adam_update(moved_params, moved_first, moved_second, gradients, clip_factor)
```

```python
import functools
import math

import jax
import jax.numpy as jnp
from jax import lax
from jax.experimental import pallas as pl
from jax.experimental.pallas import tpu as pltpu
from jax.sharding import PartitionSpec as P

STEP = 100
MESH = pl.DeviceIdType.MESH
AXES = ("row", "col")

beta_one = 0.9
beta_two = 0.95
epsilon = 1e-08
learn_rate = 0.001
decay_rate = 0.1


def flipped(index, bits):
    out = index
    for number in range(bits.bit_length()):
        size = 1 << number
        if bits & size:
            out = out + size * (1 - 2 * ((index // size) % 2))
    return out


def exchange(tensor, key, columns, s_ref, o_ref, send, recv):
    partner = (
        flipped(lax.axis_index("row"), key // columns),
        flipped(lax.axis_index("col"), key % columns),
    )
    barrier = pltpu.get_barrier_semaphore()
    pl.semaphore_signal(barrier, inc=1, device_id=partner, device_id_type=MESH)
    pl.semaphore_wait(barrier, 1)
    copy = pltpu.make_async_remote_copy(
        src_ref=s_ref,
        dst_ref=o_ref,
        send_sem=send,
        recv_sem=recv,
        device_id=partner,
        device_id_type=MESH,
    )
    copy.start()
    copy.wait()


def keep(tensor, s_ref, o_ref):
    o_ref[...] = s_ref[...]


def moved_by(tensor, key, columns, total, shape):
    if key == 0:
        return pl.pallas_call(
            functools.partial(keep, tensor),
            out_shape=jax.ShapeDtypeStruct(shape, jnp.float32),
            in_specs=[pl.BlockSpec(memory_space=pltpu.VMEM)],
            out_specs=pl.BlockSpec(memory_space=pltpu.VMEM),
            name="keep",
        )
    return pl.pallas_call(
        functools.partial(exchange, tensor, key, columns),
        out_shape=jax.ShapeDtypeStruct(shape, jnp.float32),
        in_specs=[pl.BlockSpec(memory_space=pltpu.VMEM)],
        out_specs=pl.BlockSpec(memory_space=pltpu.VMEM),
        scratch_shapes=[pltpu.SemaphoreType.DMA, pltpu.SemaphoreType.DMA],
        compiler_params=pltpu.CompilerParams(
            collective_id=key, has_side_effects=True
        ),
        name="exchange",
    )


def gather(p_ref, m_ref, v_ref, g_ref, s0_ref, s1_ref, sum_ref, sems):
    tensors = p_ref.shape[0]
    copies = []
    for number, ref in enumerate((p_ref, m_ref, v_ref)):
        for tensor, s_ref in enumerate((s0_ref, s1_ref)):
            copy = pltpu.make_async_copy(ref.at[tensor], s_ref.at[number], sems.at[tensor, number])
            copy.start()
            copies.append(copy)
    rows = g_ref.shape[1]

    def body(i, total):
        at = pl.ds(pl.multiple_of(i * 64, 64), 64)
        for tensor in range(tensors):
            g = g_ref[tensor, at, :]
            total = total + jnp.sum((g * g).reshape(8, 8, 128), axis=0)
        return total

    sum_ref[...] = lax.fori_loop(0, rows // 64, body, jnp.zeros((8, 128), jnp.float32))
    for copy in copies:
        copy.wait()


def adam_update(params, first_moment, second_moment, gradients, clip_factor):
    scaled = clip_factor * gradients
    first_new = beta_one * first_moment + (1.0 - beta_one) * scaled
    second_new = beta_two * second_moment + (1.0 - beta_two) * scaled * scaled
    bias_first = 1.0 - beta_one**STEP
    bias_second = 1.0 - beta_two**STEP
    update = first_new / bias_first / (jnp.sqrt(second_new / bias_second) + epsilon)
    params_new = params - learn_rate * (update + decay_rate * params)
    return (params_new, first_new, second_new)


def adam(swap_ref, clip_ref, *refs):
    moved, (g_ref, po_ref, mo_ref, vo_ref) = refs[:2], refs[2:]
    clip = clip_ref[0:1, 0:1]
    rows = g_ref.shape[1]
    half = rows // 2
    step = 64
    for tensor in range(2):
        state = moved[tensor]
        for side in range(2):
            first_row = jnp.bitwise_xor(swap_ref[tensor], side)

            def body(i, carry, state=state, side=side, first_row=first_row, tensor=tensor):
                values = [
                    state[number, pl.ds(first_row + 2 * i * step, step, stride=2), :]
                    for number in range(3)
                ]
                at = pl.ds(pl.multiple_of(side * half + i * step, step), step)
                new = adam_update(*values, g_ref[tensor, at, :], clip)
                for ref, value in zip((po_ref, mo_ref, vo_ref), new):
                    ref[tensor, at, :] = value
                return carry

            lax.fori_loop(0, half // step, body, 0)


def reduce_kernel(sizes, limit, part_ref, clip_ref, held, slots, send, recv):
    me = [lax.axis_index(name) for name in AXES]
    barrier = pltpu.get_barrier_semaphore()

    def peer(axis, step):
        other = lax.rem(me[axis] + step, sizes[axis])
        return (other, me[1]) if axis == 0 else (me[0], other)

    for axis in range(2):

        def greet(step, carry, axis=axis):
            pl.semaphore_signal(
                barrier, inc=1, device_id=peer(axis, step), device_id_type=MESH
            )
            return carry

        lax.fori_loop(1, sizes[axis], greet, 0)
    pl.semaphore_wait(barrier, sizes[0] + sizes[1] - 2)
    value = jnp.sum(part_ref[...], axis=0, keepdims=True)
    for axis in range(2):
        size = sizes[axis]
        held[axis] = value

        def give(step, carry, axis=axis):
            pltpu.make_async_remote_copy(
                src_ref=held.at[axis],
                dst_ref=slots.at[axis, step],
                send_sem=send.at[axis],
                recv_sem=recv.at[axis],
                device_id=peer(axis, step),
                device_id_type=MESH,
            ).start()
            return carry

        lax.fori_loop(1, size, give, 0)
        whole = pltpu.make_async_remote_copy(
            src_ref=slots.at[axis, pl.ds(1, size - 1)],
            dst_ref=slots.at[axis, pl.ds(1, size - 1)],
            send_sem=send.at[axis],
            recv_sem=recv.at[axis],
            device_id=peer(axis, 1),
            device_id_type=MESH,
        )
        whole.wait()
        for step in range(1, size):
            value = value + slots[axis, step]
    norm = jnp.sqrt(jnp.sum(value, axis=1, keepdims=True))
    clip_ref[...] = jnp.broadcast_to(limit / jnp.maximum(norm, limit), clip_ref.shape)


def global_clip(partial, sizes, count):
    most = max(sizes)
    return pl.pallas_call(
        functools.partial(reduce_kernel, sizes, 0.5 * math.sqrt(count)),
        out_shape=jax.ShapeDtypeStruct((1, 128), jnp.float32),
        in_specs=[pl.BlockSpec(memory_space=pltpu.VMEM)],
        out_specs=pl.BlockSpec(memory_space=pltpu.VMEM),
        scratch_shapes=[
            pltpu.VMEM((2, 1, 128), jnp.float32),
            pltpu.VMEM((2, most, 1, 128), jnp.float32),
            pltpu.SemaphoreType.DMA((2,)),
            pltpu.SemaphoreType.DMA((2,)),
        ],
        compiler_params=pltpu.CompilerParams(collective_id=0, has_side_effects=True),
        name="reduce",
    )(partial)


def shards(columns, total, old_params, old_first, old_second, gradients, old_table, new_table):
    old_key = old_table[:, 0]
    route_key = jnp.bitwise_xor(jnp.right_shift(old_key, 1), new_table[:, 0])
    swap = jnp.bitwise_and(old_key, 1)
    tensors, _, width = old_params.shape
    rows = 2 * width // 128

    def lined(x):
        x = x.reshape(tensors, 2, width // 128, 128)
        return x.transpose(0, 2, 1, 3).reshape(tensors, rows, 128)

    state = [lined(x) for x in (old_params, old_first, old_second)]
    gradients = gradients.reshape(tensors, rows, 128)
    *stacked, partial = pl.pallas_call(
        gather,
        out_shape=(
            jax.ShapeDtypeStruct((3, rows, 128), jnp.float32),
            jax.ShapeDtypeStruct((3, rows, 128), jnp.float32),
            jax.ShapeDtypeStruct((8, 128), jnp.float32),
        ),
        in_specs=[pl.BlockSpec(memory_space=pl.ANY)] * 3
        + [pl.BlockSpec(memory_space=pltpu.VMEM)],
        out_specs=[pl.BlockSpec(memory_space=pltpu.VMEM)] * 3,
        scratch_shapes=[pltpu.SemaphoreType.DMA((2, 3))],
        name="gather",
    )(*state, gradients)
    branches = [moved_by(0, key, columns, total, (3, rows, 128)) for key in range(total)]

    def turn(i, carry):
        first, second = carry
        return second, lax.switch(route_key[i], branches, first)

    moved = lax.fori_loop(0, tensors, turn, tuple(stacked))
    clip = global_clip(partial, (total // columns, columns), gradients.size * total)
    new = pl.pallas_call(
        adam,
        out_shape=(jax.ShapeDtypeStruct((tensors, rows, 128), jnp.float32),) * 3,
        in_specs=[pl.BlockSpec(memory_space=pltpu.SMEM)]
        + [pl.BlockSpec(memory_space=pltpu.VMEM)] * 4,
        out_specs=[pl.BlockSpec(memory_space=pltpu.VMEM)] * 3,
        name="adam",
    )(swap, clip, *moved, gradients)
    return tuple(x.reshape(tensors, 1, rows * 128) for x in new)


def solution(mesh):
    columns = mesh.shape["col"]
    total = mesh.size
    split = P(None, AXES, None)
    return jax.shard_map(
        functools.partial(shards, columns, total),
        mesh=mesh,
        in_specs=(split,) * 4 + (P(), P()),
        out_specs=(split,) * 3,
        check_vma=False,
    )
```

```python
import functools
import math

import jax
import jax.numpy as jnp
from jax import lax
from jax.experimental import pallas as pl
from jax.experimental.pallas import tpu as pltpu
from jax.sharding import PartitionSpec as P

STEP = 100
MESH = pl.DeviceIdType.MESH
AXES = ("row", "col")
LANES = 128
SUBLANES = 8

beta_one = 0.9
beta_two = 0.95
epsilon = 1e-08
learn_rate = 0.001
decay_rate = 0.1

STAGE = 7


def stage_masks(member, far):
    scale = 3 if far else 1
    return (((member & 1) * 4 + ((member >> 1) & 1)) * scale, (member >> 2) * 2 * scale)


STAGE_MASKS = {stage_masks(member, far) for far in range(2) for member in range(1, STAGE + 1)}


def flip(index, bits):
    return jnp.bitwise_xor(index, bits)


def by_rows(rows, step, move):
    def body(i, carry):
        move(pl.ds(pl.multiple_of(i * step, step), step))
        return carry

    lax.fori_loop(0, rows // step, body, 0)


def exchange(row_key, odd, s_ref, v_ref, o_ref, t_ref, landed, slots, small, bulk, sides):
    row, col = lax.axis_index("row"), lax.axis_index("col")
    planes, rows, _ = s_ref.shape[1:]
    barrier = pltpu.get_barrier_semaphore()
    masks = (((0, 2), 0), ((0, 6), 1)) if odd else (((0, 4), 1),)
    extra = [mask for mask, _ in masks if mask not in STAGE_MASKS]
    if row_key and (row_key, 0) not in STAGE_MASKS:
        extra.append((row_key, 0))

    def at(mask):
        return (flip(row, mask[0]), flip(col, mask[1]))

    for mask in extra:
        pl.semaphore_signal(barrier, inc=1, device_id=at(mask), device_id_type=MESH)

    def greet(member, carry):
        for far in range(2):
            peer = at(stage_masks(member, far))
            pl.semaphore_signal(barrier, inc=1, device_id=peer, device_id_type=MESH)
        return carry

    lax.fori_loop(1, STAGE + 1, greet, 0)
    pl.semaphore_wait(barrier, 2 * STAGE + len(extra))

    def give(member, carry):
        for far in range(2):
            pltpu.make_async_remote_copy(
                src_ref=v_ref.at[0],
                dst_ref=slots.at[far, member - 1],
                send_sem=small.at[0],
                recv_sem=small.at[1],
                device_id=at(stage_masks(member, far)),
                device_id_type=MESH,
            ).start()
        return carry

    lax.fori_loop(1, STAGE + 1, give, 0)
    across = []
    for mask, place in masks:
        across.append(
            pltpu.make_async_remote_copy(
                src_ref=s_ref.at[1],
                dst_ref=landed.at[place],
                send_sem=sides.at[0, place],
                recv_sem=sides.at[1, place],
                device_id=at(mask),
                device_id_type=MESH,
            )
        )
    if row_key:
        straight = pltpu.make_async_remote_copy(
            src_ref=s_ref.at[0],
            dst_ref=o_ref.at[1],
            send_sem=bulk.at[0],
            recv_sem=bulk.at[1],
            device_id=at((row_key, 0)),
            device_id_type=MESH,
        )
        straight.start()
    for copy in across:
        copy.start()
    if not row_key:

        def keep(part):
            for plane in range(planes):
                o_ref[1, plane, part, :] = s_ref[0, plane, part, :]

        by_rows(rows, 64, keep)
    pltpu.make_async_remote_copy(
        src_ref=slots,
        dst_ref=slots,
        send_sem=small.at[0],
        recv_sem=small.at[1],
        device_id=at((1, 0)),
        device_id_type=MESH,
    ).wait()
    t_ref[0:2] = v_ref[0][None] + jnp.sum(slots[...], axis=1)
    t_ref[2] = v_ref[3]
    t_ref[3] = v_ref[2]
    chosen = v_ref[2] > 0.5
    for copy in across:
        copy.wait()

    def pick(part):
        for plane in range(planes):
            other = landed[0, plane, part, :] if odd else s_ref[1, plane, part, :]
            o_ref[0, plane, part, :] = jnp.where(chosen, landed[1, plane, part, :], other)

    by_rows(rows, 64, pick)
    if row_key:
        straight.wait()


def exchanged(row_key, odd, state, value):
    whole = pl.BlockSpec(memory_space=pltpu.VMEM)
    return pl.pallas_call(
        functools.partial(exchange, row_key, odd),
        out_shape=(state, value),
        in_specs=[whole] * 2,
        out_specs=[whole] * 2,
        scratch_shapes=[
            pltpu.VMEM(state.shape, jnp.float32),
            pltpu.VMEM((2, STAGE, 1, LANES), jnp.float32),
            pltpu.SemaphoreType.DMA((2,)),
            pltpu.SemaphoreType.DMA((2,)),
            pltpu.SemaphoreType.DMA((2, 2)),
        ],
        compiler_params=pltpu.CompilerParams(
            collective_id=2 * row_key + odd, has_side_effects=True
        ),
        name="exchange",
    )


def gather(
    p_ref, m_ref, v_ref, g_hbm, old_hbm, new_hbm,
    s_ref, g_ref, t_ref, key_ref,
    both, old_smem, new_smem, sums, sems, state_sems, core_sems,
):
    row, col = lax.axis_index("row"), lax.axis_index("col")
    twin = (row, flip(col, 1))
    barrier = pltpu.get_barrier_semaphore()
    pl.semaphore_signal(barrier, inc=1, device_id=twin, device_id_type=MESH)
    smalls = [
        pltpu.make_async_copy(old_hbm.at[:, pl.ds(0, LANES)], old_smem, sems.at[0]),
        pltpu.make_async_copy(new_hbm.at[:, pl.ds(0, LANES)], new_smem, sems.at[1]),
    ]
    gradient = pltpu.make_async_copy(g_hbm, g_ref, sems.at[2])
    gradient.start()
    for copy in smalls:
        copy.start()
    copies = []
    for number, source in enumerate((p_ref, m_ref, v_ref)):
        copies.append(
            pltpu.make_async_copy(source, both.at[0, :, number], state_sems.at[0, number])
        )
        copies[-1].start()
    pl.semaphore_wait(barrier, 1)
    for number, source in enumerate((p_ref, m_ref, v_ref)):
        copies.append(
            pltpu.make_async_remote_copy(
                src_ref=source,
                dst_ref=both.at[1, :, number],
                send_sem=state_sems.at[1, number],
                recv_sem=state_sems.at[2, number],
                device_id=twin,
                device_id_type=MESH,
            )
        )
        copies[-1].start()
    gradient.wait()
    tensors, length, _ = g_ref.shape
    step = 64

    def body(i, total):
        at = pl.ds(pl.multiple_of(i * step, step), step)
        for tensor in range(tensors):
            g = g_ref[tensor, at, :].reshape(step // SUBLANES, SUBLANES, LANES)
            total = total + jnp.sum(g * g, axis=0)
        return total

    total = lax.fori_loop(0, length // step, body, jnp.zeros((SUBLANES, LANES), jnp.float32))
    sums[0] = jnp.sum(total, axis=0, keepdims=True)
    swap = pltpu.make_async_remote_copy(
        src_ref=sums.at[0],
        dst_ref=sums.at[1],
        send_sem=core_sems.at[0],
        recv_sem=core_sems.at[1],
        device_id=twin,
        device_id_type=MESH,
    )
    swap.start()
    for copy in smalls:
        copy.wait()
    rows, odds, cores = [], [], []
    for tensor in range(2):
        old = old_smem[tensor, 0]
        route = jnp.bitwise_xor(jnp.right_shift(old, 1), new_smem[tensor, 0])
        key_y = jnp.bitwise_and(jnp.right_shift(route, 1), 3)
        odd = jnp.bitwise_and(key_y, 1)
        second = jnp.where(key_y >= 2, 1.0, 0.0)
        rows.append(jnp.right_shift(route, 3))
        odds.append(odd)
        cores.append(jnp.bitwise_and(route, 1))
        key_ref[2 + tensor] = jnp.bitwise_and(old, 1)
        t_ref[3 - tensor] = jnp.full((1, LANES), second, jnp.float32)
    key_ref[0] = 2 * rows[0] + odds[1]
    key_ref[1] = 2 * rows[1] + odds[0]
    for copy in copies:
        copy.wait()
    for tensor in range(2):

        def pick(part, tensor=tensor):
            for plane in range(3):
                s_ref[tensor, plane, part, :] = both[cores[tensor], tensor, plane, part, :]

        by_rows(length, 64, pick)
    swap.wait()
    t_ref[0] = sums[0] + sums[1]
    t_ref[1] = sums[0] + sums[1]


def adam_update(params, first_moment, second_moment, gradients, clip_factor):
    scaled = clip_factor * gradients
    first_new = beta_one * first_moment + (1.0 - beta_one) * scaled
    second_new = beta_two * second_moment + (1.0 - beta_two) * scaled * scaled
    bias_first = 1.0 - beta_one**STEP
    bias_second = 1.0 - beta_two**STEP
    update = first_new * (1.0 / bias_first) / (jnp.sqrt(second_new * (1.0 / bias_second)) + epsilon)
    params_new = params - learn_rate * (update + decay_rate * params)
    return (params_new, first_new, second_new)


def adam(limit, key_ref, sum_ref, s_ref, g_ref, po_hbm, mo_hbm, vo_hbm, po_ref, mo_ref, vo_ref, sems):
    squares = jnp.full((SUBLANES, LANES), jnp.sum(sum_ref[1]), jnp.float32)
    clip = limit / jnp.maximum(jnp.sqrt(squares), limit)
    length = g_ref.shape[1]
    half = length // 2
    step = 64
    tile = (step // SUBLANES, SUBLANES, LANES)
    copies = []
    for tensor in range(2):
        for side in range(2):
            first_row = jnp.bitwise_xor(key_ref[2 + tensor], side)

            def body(i, carry, side=side, first_row=first_row, tensor=tensor):
                part = pl.ds(first_row + 2 * i * step, step, stride=2)
                values = [s_ref[tensor, number, part, :].reshape(tile) for number in range(3)]
                at = pl.ds(pl.multiple_of(side * half + i * step, step), step)
                new = adam_update(*values, g_ref[tensor, at, :].reshape(tile), clip[None])
                for ref, value in zip((po_ref, mo_ref, vo_ref), new):
                    ref[tensor, at, :] = value.reshape(step, LANES)
                return carry

            lax.fori_loop(0, half // step, body, 0)
            part = pl.ds(side * half, half)
            for number, (source, target) in enumerate(
                ((po_ref, po_hbm), (mo_ref, mo_hbm), (vo_ref, vo_hbm))
            ):
                copy = pltpu.make_async_copy(
                    source.at[tensor, part], target.at[tensor, part], sems.at[tensor, side, number]
                )
                copy.start()
                copies.append(copy)
    for copy in copies:
        copy.wait()


def shards(total, old_params, old_first, old_second, gradients, old_table, new_table):
    tensors, _, width = old_params.shape
    rows = 2 * width // LANES

    def lined(x):
        x = x.reshape(tensors, 2, width // LANES, LANES)
        return x.transpose(0, 2, 1, 3).reshape(tensors, rows, LANES)

    anywhere = pl.BlockSpec(memory_space=pl.ANY)
    whole = pl.BlockSpec(memory_space=pltpu.VMEM)
    scalars = pl.BlockSpec(memory_space=pltpu.SMEM)
    state = jax.ShapeDtypeStruct((tensors, 3, rows, LANES), jnp.float32)
    value = jax.ShapeDtypeStruct((4, 1, LANES), jnp.float32)
    full = jax.ShapeDtypeStruct((tensors, rows, LANES), jnp.float32)
    variants = [(row_key, odd) for row_key in range(16) for odd in range(2)]
    stacked, gradient, shared, keys = pl.pallas_call(
        gather,
        out_shape=(state, full, value, jax.ShapeDtypeStruct((4,), jnp.int32)),
        in_specs=[anywhere] * 6,
        out_specs=[whole] * 3 + [scalars],
        scratch_shapes=[
            pltpu.VMEM((2, *state.shape), jnp.float32),
            pltpu.SMEM((tensors, LANES), jnp.int32),
            pltpu.SMEM((tensors, LANES), jnp.int32),
            pltpu.VMEM((2, 1, LANES), jnp.float32),
            pltpu.SemaphoreType.DMA((3,)),
            pltpu.SemaphoreType.DMA((3, 3)),
            pltpu.SemaphoreType.DMA((2,)),
        ],
        compiler_params=pltpu.CompilerParams(
            collective_id=len(variants), has_side_effects=True
        ),
        name="gather",
    )(
        *(lined(x) for x in (old_params, old_first, old_second)),
        gradients.reshape(tensors, rows, LANES),
        old_table,
        new_table,
    )
    branches = [exchanged(row_key, odd, state, value) for row_key, odd in variants]

    def turn(i, carry):
        return tuple(lax.switch(keys[i], branches, *carry))

    stacked, shared = lax.fori_loop(0, tensors, turn, (stacked, shared))
    new = pl.pallas_call(
        functools.partial(adam, 0.5 * math.sqrt(gradients.size * total)),
        out_shape=(full,) * 3,
        in_specs=[scalars] + [whole] * 3,
        out_specs=[anywhere] * 3,
        scratch_shapes=[pltpu.VMEM(full.shape, jnp.float32)] * 3
        + [pltpu.SemaphoreType.DMA((tensors, 2, 3))],
        name="adam",
    )(keys, shared, stacked, gradient)
    return tuple(x.reshape(tensors, 1, rows * LANES) for x in new)


def solution(mesh):
    split = P(None, AXES, None)
    return jax.shard_map(
        functools.partial(shards, mesh.size),
        mesh=mesh,
        in_specs=(split,) * 4 + (P(), P()),
        out_specs=(split,) * 3,
        check_vma=False,
    )
```

```python
import functools
import math

import jax
import jax.numpy as jnp
from jax import lax
from jax.experimental import pallas as pl
from jax.experimental.pallas import tpu as pltpu
from jax.sharding import PartitionSpec as P

STEP = 100
MESH = pl.DeviceIdType.MESH
AXES = ("row", "col")
LANES = 128
SUBLANES = 8

beta_one = 0.9
beta_two = 0.95
epsilon = 1e-08
learn_rate = 0.001
decay_rate = 0.1

STAGE = 7


def stage_masks(member, far):
    scale = 3 if far else 1
    return (((member & 1) * 4 + ((member >> 1) & 1)) * scale, (member >> 2) * 2 * scale)


STAGE_MASKS = {stage_masks(member, far) for far in range(2) for member in range(1, STAGE + 1)}


def flip(index, bits):
    return jnp.bitwise_xor(index, bits)


def by_rows(rows, step, move):
    def body(i, carry):
        move(pl.ds(pl.multiple_of(i * step, step), step))
        return carry

    lax.fori_loop(0, rows // step, body, 0)


def exchange(row_key, odd, s_ref, v_ref, o_ref, t_ref, landed, slots, small, bulk, sides):
    row, col = lax.axis_index("row"), lax.axis_index("col")
    planes, rows, _ = s_ref.shape[1:]
    barrier = pltpu.get_barrier_semaphore()
    masks = (((0, 2), 0), ((0, 6), 1)) if odd else (((0, 4), 1),)
    extra = [mask for mask, _ in masks if mask not in STAGE_MASKS]
    if row_key and (row_key, 0) not in STAGE_MASKS:
        extra.append((row_key, 0))

    def at(mask):
        return (flip(row, mask[0]), flip(col, mask[1]))

    for mask in extra:
        pl.semaphore_signal(barrier, inc=1, device_id=at(mask), device_id_type=MESH)

    def greet(member, carry):
        for far in range(2):
            peer = at(stage_masks(member, far))
            pl.semaphore_signal(barrier, inc=1, device_id=peer, device_id_type=MESH)
        return carry

    lax.fori_loop(1, STAGE + 1, greet, 0)
    pl.semaphore_wait(barrier, 2 * STAGE + len(extra))

    def give(member, carry):
        for far in range(2):
            pltpu.make_async_remote_copy(
                src_ref=v_ref.at[0],
                dst_ref=slots.at[far, member - 1],
                send_sem=small.at[0],
                recv_sem=small.at[1],
                device_id=at(stage_masks(member, far)),
                device_id_type=MESH,
            ).start()
        return carry

    lax.fori_loop(1, STAGE + 1, give, 0)
    across = []
    for mask, place in masks:
        across.append(
            pltpu.make_async_remote_copy(
                src_ref=s_ref.at[1],
                dst_ref=landed.at[place],
                send_sem=sides.at[0, place],
                recv_sem=sides.at[1, place],
                device_id=at(mask),
                device_id_type=MESH,
            )
        )
    if row_key:
        straight = pltpu.make_async_remote_copy(
            src_ref=s_ref.at[0],
            dst_ref=o_ref.at[1],
            send_sem=bulk.at[0],
            recv_sem=bulk.at[1],
            device_id=at((row_key, 0)),
            device_id_type=MESH,
        )
        straight.start()
    for copy in across:
        copy.start()
    if not row_key:

        def keep(part):
            for plane in range(planes):
                o_ref[1, plane, part, :] = s_ref[0, plane, part, :]

        by_rows(rows, 64, keep)
    pltpu.make_async_remote_copy(
        src_ref=slots,
        dst_ref=slots,
        send_sem=small.at[0],
        recv_sem=small.at[1],
        device_id=at((1, 0)),
        device_id_type=MESH,
    ).wait()
    t_ref[0:2] = v_ref[0][None] + jnp.sum(slots[...], axis=1)
    t_ref[2] = v_ref[3]
    t_ref[3] = v_ref[2]
    t_ref[4:6] = v_ref[4:6]
    chosen = v_ref[2] > 0.5
    for copy in across:
        copy.wait()

    def pick(part):
        for plane in range(planes):
            other = landed[0, plane, part, :] if odd else s_ref[1, plane, part, :]
            o_ref[0, plane, part, :] = jnp.where(chosen, landed[1, plane, part, :], other)

    by_rows(rows, 64, pick)
    if row_key:
        straight.wait()


def exchanged(row_key, odd, state, value):
    whole = pl.BlockSpec(memory_space=pltpu.VMEM)
    return pl.pallas_call(
        functools.partial(exchange, row_key, odd),
        out_shape=(state, value),
        in_specs=[whole] * 2,
        out_specs=[whole] * 2,
        scratch_shapes=[
            pltpu.VMEM(state.shape, jnp.float32),
            pltpu.VMEM((2, STAGE, 1, LANES), jnp.float32),
            pltpu.SemaphoreType.DMA((2,)),
            pltpu.SemaphoreType.DMA((2,)),
            pltpu.SemaphoreType.DMA((2, 2)),
        ],
        compiler_params=pltpu.CompilerParams(
            collective_id=2 * row_key + odd, has_side_effects=True
        ),
        name="exchange",
    )


def gather(
    p_ref, m_ref, v_ref, g_hbm, old_hbm, new_hbm,
    s_ref, t_ref, key0_hbm, key1_hbm,
    g_ref, both, old_smem, new_smem, key_smem, sums, sems, state_sems, core_sems,
):
    row, col = lax.axis_index("row"), lax.axis_index("col")
    twin = (row, flip(col, 1))
    barrier = pltpu.get_barrier_semaphore()
    pl.semaphore_signal(barrier, inc=1, device_id=twin, device_id_type=MESH)
    smalls = [
        pltpu.make_async_copy(old_hbm.at[:, pl.ds(0, LANES)], old_smem, sems.at[0]),
        pltpu.make_async_copy(new_hbm.at[:, pl.ds(0, LANES)], new_smem, sems.at[1]),
    ]
    gradient = pltpu.make_async_copy(g_hbm, g_ref, sems.at[2])
    gradient.start()
    for copy in smalls:
        copy.start()
    copies = []
    for number, source in enumerate((p_ref, m_ref, v_ref)):
        copies.append(
            pltpu.make_async_copy(source, both.at[0, :, number], state_sems.at[0, number])
        )
        copies[-1].start()
    pl.semaphore_wait(barrier, 1)
    for number, source in enumerate((p_ref, m_ref, v_ref)):
        copies.append(
            pltpu.make_async_remote_copy(
                src_ref=source,
                dst_ref=both.at[1, :, number],
                send_sem=state_sems.at[1, number],
                recv_sem=state_sems.at[2, number],
                device_id=twin,
                device_id_type=MESH,
            )
        )
        copies[-1].start()
    gradient.wait()
    tensors, length, _ = g_ref.shape
    step = 64

    def body(i, total):
        at = pl.ds(pl.multiple_of(i * step, step), step)
        for tensor in range(tensors):
            g = g_ref[tensor, at, :].reshape(step // SUBLANES, SUBLANES, LANES)
            total = total + jnp.sum(g * g, axis=0)
        return total

    total = lax.fori_loop(0, length // step, body, jnp.zeros((SUBLANES, LANES), jnp.float32))
    sums[0] = jnp.sum(total, axis=0, keepdims=True)
    swap = pltpu.make_async_remote_copy(
        src_ref=sums.at[0],
        dst_ref=sums.at[1],
        send_sem=core_sems.at[0],
        recv_sem=core_sems.at[1],
        device_id=twin,
        device_id_type=MESH,
    )
    swap.start()
    for copy in smalls:
        copy.wait()
    rows, odds, cores = [], [], []
    for tensor in range(2):
        old = old_smem[tensor, 0]
        route = jnp.bitwise_xor(jnp.right_shift(old, 1), new_smem[tensor, 0])
        key_y = jnp.bitwise_and(jnp.right_shift(route, 1), 3)
        odd = jnp.bitwise_and(key_y, 1)
        second = jnp.where(key_y >= 2, 1.0, 0.0)
        rows.append(jnp.right_shift(route, 3))
        odds.append(odd)
        cores.append(jnp.bitwise_and(route, 1))
        t_ref[3 - tensor] = jnp.full((1, LANES), second, jnp.float32)
        swapped = jnp.where(jnp.bitwise_and(old, 1) == 1, 1.0, 0.0)
        t_ref[4 + tensor] = jnp.full((1, LANES), swapped, jnp.float32)
    for turn, target in enumerate((key0_hbm, key1_hbm)):
        key_smem[turn, 0] = 2 * rows[turn] + odds[1 - turn]
        copies.append(pltpu.make_async_copy(key_smem.at[turn], target, sems.at[3 + turn]))
        copies[-1].start()
    for number in range(3):
        for copy in copies[number : 2 * 3 : 3]:
            copy.wait()

        def pick(part, number=number):
            for tensor in range(tensors):
                s_ref[tensor, number, part, :] = jnp.where(
                    cores[tensor] == 1,
                    both[1, tensor, number, part, :],
                    both[0, tensor, number, part, :],
                )

        by_rows(length, 64, pick)
    for copy in copies[2 * 3 :]:
        copy.wait()
    swap.wait()
    t_ref[0] = sums[0] + sums[1]
    t_ref[1] = sums[0] + sums[1]


def adam_update(params, first_moment, second_moment, gradients, clip_factor):
    scaled = clip_factor * gradients
    first_new = beta_one * first_moment + (1.0 - beta_one) * scaled
    second_new = beta_two * second_moment + (1.0 - beta_two) * scaled * scaled
    bias_first = 1.0 - beta_one**STEP
    bias_second = 1.0 - beta_two**STEP
    update = first_new * (1.0 / bias_first) / (jnp.sqrt(second_new * (1.0 / bias_second)) + epsilon)
    params_new = params - learn_rate * (update + decay_rate * params)
    return (params_new, first_new, second_new)


def adam(limit, t_ref, s_ref, g_ref, po_hbm, mo_hbm, vo_hbm, po_ref, mo_ref, vo_ref, sems):
    squares = jnp.full((SUBLANES, LANES), jnp.sum(t_ref[1]), jnp.float32)
    clip = limit / jnp.maximum(jnp.sqrt(squares), limit)
    length = g_ref.shape[1]
    half = length // 2
    step = 32
    tile = (step // SUBLANES, SUBLANES, LANES)
    copies = []
    for tensor in range(2):
        crossed = jnp.broadcast_to(t_ref[4 + tensor], (SUBLANES, LANES))[None] > 0.5

        def body(i, carry, crossed=crossed, tensor=tensor):
            halves = [
                [
                    s_ref[tensor, number, pl.ds(side + 2 * i * step, step, stride=2), :].reshape(tile)
                    for number in range(3)
                ]
                for side in range(2)
            ]
            for side in range(2):
                at = pl.ds(pl.multiple_of(side * half + i * step, step), step)
                values = [
                    jnp.where(crossed, other, own)
                    for own, other in zip(halves[side], halves[1 - side])
                ]
                new = adam_update(*values, g_ref[tensor, at, :].reshape(tile), clip[None])
                for ref, value in zip((po_ref, mo_ref, vo_ref), new):
                    ref[tensor, at, :] = value.reshape(step, LANES)
            return carry

        parts = 2
        for part in range(parts):
            steps = half // step // parts
            lax.fori_loop(part * steps, (part + 1) * steps, body, 0)
            for side in range(2):
                at = pl.ds(side * half + part * steps * step, steps * step)
                for number, (source, target) in enumerate(
                    ((po_ref, po_hbm), (mo_ref, mo_hbm), (vo_ref, vo_hbm))
                ):
                    copy = pltpu.make_async_copy(
                        source.at[tensor, at],
                        target.at[tensor, at],
                        sems.at[tensor, part, side, number],
                    )
                    copy.start()
                    copies.append(copy)
    for copy in copies:
        copy.wait()


def chosen_branch(index, branches, *operands):
    traced = jax.make_jaxpr(lambda i, *xs: lax.switch(i, branches, *xs))(index, *operands)
    choice = traced.eqns[-1]
    return choice.primitive.bind(index, *operands, **choice.params)


def shards(total, old_params, old_first, old_second, gradients, old_table, new_table):
    tensors, _, width = old_params.shape
    rows = 2 * width // LANES

    def lined(x):
        x = x.reshape(tensors, 2, width // LANES, LANES)
        return x.transpose(0, 2, 1, 3).reshape(tensors, rows, LANES)

    anywhere = pl.BlockSpec(memory_space=pl.ANY)
    whole = pl.BlockSpec(memory_space=pltpu.VMEM)
    state = jax.ShapeDtypeStruct((tensors, 3, rows, LANES), jnp.float32)
    value = jax.ShapeDtypeStruct((6, 1, LANES), jnp.float32)
    key = jax.ShapeDtypeStruct((1,), jnp.int32)
    full = jax.ShapeDtypeStruct((tensors, rows, LANES), jnp.float32)
    variants = [(row_key, odd) for row_key in range(16) for odd in range(2)]
    gradients = gradients.reshape(tensors, rows, LANES)
    stacked, shared, *keys = pl.pallas_call(
        gather,
        out_shape=(state, value, key, key),
        in_specs=[anywhere] * 6,
        out_specs=[whole] * 2 + [anywhere] * 2,
        scratch_shapes=[
            pltpu.VMEM(full.shape, jnp.float32),
            pltpu.VMEM((2, *state.shape), jnp.float32),
            pltpu.SMEM((tensors, LANES), jnp.int32),
            pltpu.SMEM((tensors, LANES), jnp.int32),
            pltpu.SMEM((2, 1), jnp.int32),
            pltpu.VMEM((2, 1, LANES), jnp.float32),
            pltpu.SemaphoreType.DMA((5,)),
            pltpu.SemaphoreType.DMA((3, 3)),
            pltpu.SemaphoreType.DMA((2,)),
        ],
        compiler_params=pltpu.CompilerParams(
            collective_id=len(variants), has_side_effects=True
        ),
        name="gather",
    )(
        *(lined(x) for x in (old_params, old_first, old_second)),
        gradients,
        old_table,
        new_table,
    )
    branches = [exchanged(row_key, odd, state, value) for row_key, odd in variants]

    for key in keys:
        stacked, shared = chosen_branch(key.reshape(()), branches, stacked, shared)
    new = pl.pallas_call(
        functools.partial(adam, 0.5 * math.sqrt(gradients.size * total)),
        out_shape=(full,) * 3,
        in_specs=[whole] * 3,
        out_specs=[anywhere] * 3,
        scratch_shapes=[pltpu.VMEM(full.shape, jnp.float32)] * 3
        + [pltpu.SemaphoreType.DMA((tensors, 2, 2, 3))],
        name="adam",
    )(shared, stacked, gradients)
    return tuple(x.reshape(tensors, 1, rows * LANES) for x in new)


def solution(mesh):
    split = P(None, AXES, None)
    return jax.shard_map(
        functools.partial(shards, mesh.size),
        mesh=mesh,
        in_specs=(split,) * 4 + (P(), P()),
        out_specs=(split,) * 3,
        check_vma=False,
    )
```

```python
import functools
import math

import jax
import jax.numpy as jnp
from jax import lax
from jax.experimental import pallas as pl
from jax.experimental.pallas import tpu as pltpu
from jax.sharding import PartitionSpec as P

STEP = 100
MESH = pl.DeviceIdType.MESH
AXES = ("row", "col")
LANES = 128
SUBLANES = 8

beta_one = 0.9
beta_two = 0.95
epsilon = 1e-08
learn_rate = 0.001
decay_rate = 0.1

STAGE = 7


def stage_masks(member, far):
    scale = 3 if far else 1
    return (((member & 1) * 4 + ((member >> 1) & 1)) * scale, (member >> 2) * 2 * scale)


def flip(index, bits):
    return jnp.bitwise_xor(index, bits)


def by_rows(rows, step, move):
    def body(i, carry):
        move(pl.ds(pl.multiple_of(i * step, step), step))
        return carry

    lax.fori_loop(0, rows // step, body, 0)


def exchange(
    row_key, odd, s_ref, v_ref, o_ref, t_ref, landed, slots, go, small, tell, bulk, sides
):
    row, col = lax.axis_index("row"), lax.axis_index("col")
    planes, rows, _ = s_ref.shape[1:]
    core = col % 2
    twin = (row, flip(col, 1))
    barrier = pltpu.get_barrier_semaphore()
    sides_of = (((0, 2), 0), ((0, 6), 1)) if odd else (((0, 4), 1),)
    partners = [mask for mask, _ in sides_of]
    if row_key:
        partners.append((row_key, 0))

    def at(mask):
        return (flip(row, mask[0]), flip(col, mask[1]))

    for mask in partners:
        other_row, other_col = at(mask)
        pl.semaphore_signal(
            barrier, inc=1, device_id=(other_row, other_col + 1 - core), device_id_type=MESH
        )

    @pl.when(core == 1)
    def _():
        pl.semaphore_wait(barrier, 2 * len(partners) + 1)
        pl.semaphore_signal(go, inc=1, device_id=twin, device_id_type=MESH)

    @pl.when(core == 0)
    def _():
        pl.semaphore_signal(barrier, inc=1, device_id=twin, device_id_type=MESH)
        pl.semaphore_wait(go, 1)

    streams = []
    if row_key:
        streams.append((0, o_ref.at[1], bulk, (row_key, 0)))
    for mask, place in sides_of:
        streams.append((1, landed.at[place], sides.at[place], mask))
    copies = [
        [
            pltpu.make_async_remote_copy(
                src_ref=s_ref.at[tensor, plane],
                dst_ref=target.at[plane],
                send_sem=sems.at[0, plane],
                recv_sem=sems.at[1, plane],
                device_id=at(mask),
                device_id_type=MESH,
            )
            for tensor, target, sems, mask in streams
        ]
        for plane in range(planes)
    ]
    for plane in copies[:2]:
        for copy in plane:
            copy.start()

    @pl.when(core == 0)
    def _():
        def greet(member, carry):
            for far in range(2):
                peer = at(stage_masks(member, far))
                pl.semaphore_signal(barrier, inc=1, device_id=peer, device_id_type=MESH)
            return carry

        lax.fori_loop(1, STAGE + 1, greet, 0)
        for copy in copies[0]:
            copy.wait_send()
        pl.semaphore_wait(barrier, 2 * STAGE)

        def give(member, carry):
            for far in range(2):
                pltpu.make_async_remote_copy(
                    src_ref=v_ref.at[0],
                    dst_ref=slots.at[far, member - 1],
                    send_sem=small.at[0],
                    recv_sem=small.at[1],
                    device_id=at(stage_masks(member, far)),
                    device_id_type=MESH,
                ).start()
            return carry

        lax.fori_loop(1, STAGE + 1, give, 0)

    for copy in copies[2]:
        copy.start()
    if not row_key:

        def keep(part):
            for plane in range(planes):
                o_ref[1, plane, part, :] = s_ref[0, plane, part, :]

        by_rows(rows, 64, keep)
    forward = pltpu.make_async_remote_copy(
        src_ref=slots,
        dst_ref=slots,
        send_sem=tell.at[0],
        recv_sem=tell.at[1],
        device_id=twin,
        device_id_type=MESH,
    )

    @pl.when(core == 0)
    def _():
        pltpu.make_async_remote_copy(
            src_ref=slots,
            dst_ref=slots,
            send_sem=small.at[0],
            recv_sem=small.at[1],
            device_id=twin,
            device_id_type=MESH,
        ).wait()
        forward.start()
        forward.wait_send()

    @pl.when(core == 1)
    def _():
        forward.wait_recv()
        for copy in copies[0]:
            copy.wait_send()

    t_ref[0:2] = v_ref[0][None] + jnp.sum(slots[...], axis=1)
    t_ref[2] = v_ref[3]
    t_ref[3] = v_ref[2]
    t_ref[4:6] = v_ref[4:6]
    chosen = v_ref[2] > 0.5
    across = 1 if row_key else 0
    for plane in copies:
        for copy in plane[across:]:
            copy.wait_recv()

    def pick(part):
        for plane in range(planes):
            other = landed[0, plane, part, :] if odd else s_ref[1, plane, part, :]
            o_ref[0, plane, part, :] = jnp.where(chosen, landed[1, plane, part, :], other)

    by_rows(rows, 64, pick)
    for plane in copies:
        for copy in plane[:across]:
            copy.wait_recv()
    for plane in copies[1:]:
        for copy in plane:
            copy.wait_send()


def exchanged(row_key, odd, state, value):
    whole = pl.BlockSpec(memory_space=pltpu.VMEM)
    return pl.pallas_call(
        functools.partial(exchange, row_key, odd),
        out_shape=(state, value),
        in_specs=[whole] * 2,
        out_specs=[whole] * 2,
        scratch_shapes=[
            pltpu.VMEM(state.shape, jnp.float32),
            pltpu.VMEM((2, STAGE, 1, LANES), jnp.float32),
            pltpu.SemaphoreType.REGULAR,
            pltpu.SemaphoreType.DMA((2,)),
            pltpu.SemaphoreType.DMA((2,)),
            pltpu.SemaphoreType.DMA((2, 3)),
            pltpu.SemaphoreType.DMA((2, 2, 3)),
        ],
        compiler_params=pltpu.CompilerParams(
            collective_id=2 * row_key + odd, has_side_effects=True
        ),
        name="exchange",
    )


def gather(
    p_ref, m_ref, v_ref, g_hbm, old_hbm, new_hbm,
    s_ref, t_ref, key0_hbm, key1_hbm,
    g_ref, both, old_smem, new_smem, key_smem, sums, sems, state_sems, core_sems,
):
    row, col = lax.axis_index("row"), lax.axis_index("col")
    twin = (row, flip(col, 1))
    barrier = pltpu.get_barrier_semaphore()
    pl.semaphore_signal(barrier, inc=1, device_id=twin, device_id_type=MESH)
    smalls = [
        pltpu.make_async_copy(old_hbm.at[:, pl.ds(0, LANES)], old_smem, sems.at[0]),
        pltpu.make_async_copy(new_hbm.at[:, pl.ds(0, LANES)], new_smem, sems.at[1]),
    ]
    gradient = pltpu.make_async_copy(g_hbm, g_ref, sems.at[2])
    gradient.start()
    for copy in smalls:
        copy.start()
    copies = []
    for number, source in enumerate((p_ref, m_ref, v_ref)):
        copies.append(
            pltpu.make_async_copy(source, both.at[0, :, number], state_sems.at[0, number])
        )
        copies[-1].start()
    pl.semaphore_wait(barrier, 1)
    for number, source in enumerate((p_ref, m_ref, v_ref)):
        copies.append(
            pltpu.make_async_remote_copy(
                src_ref=source,
                dst_ref=both.at[1, :, number],
                send_sem=state_sems.at[1, number],
                recv_sem=state_sems.at[2, number],
                device_id=twin,
                device_id_type=MESH,
            )
        )
        copies[-1].start()
    gradient.wait()
    tensors, length, _ = g_ref.shape
    step = 64

    def body(i, total):
        at = pl.ds(pl.multiple_of(i * step, step), step)
        for tensor in range(tensors):
            g = g_ref[tensor, at, :].reshape(step // SUBLANES, SUBLANES, LANES)
            total = total + jnp.sum(g * g, axis=0)
        return total

    total = lax.fori_loop(0, length // step, body, jnp.zeros((SUBLANES, LANES), jnp.float32))
    sums[0] = jnp.sum(total, axis=0, keepdims=True)
    swap = pltpu.make_async_remote_copy(
        src_ref=sums.at[0],
        dst_ref=sums.at[1],
        send_sem=core_sems.at[0],
        recv_sem=core_sems.at[1],
        device_id=twin,
        device_id_type=MESH,
    )
    swap.start()
    for copy in smalls:
        copy.wait()
    rows, odds, cores = [], [], []
    for tensor in range(2):
        old = old_smem[tensor, 0]
        route = jnp.bitwise_xor(jnp.right_shift(old, 1), new_smem[tensor, 0])
        key_y = jnp.bitwise_and(jnp.right_shift(route, 1), 3)
        odd = jnp.bitwise_and(key_y, 1)
        second = jnp.where(key_y >= 2, 1.0, 0.0)
        rows.append(jnp.right_shift(route, 3))
        odds.append(odd)
        cores.append(jnp.bitwise_and(route, 1))
        t_ref[3 - tensor] = jnp.full((1, LANES), second, jnp.float32)
        swapped = jnp.where(jnp.bitwise_and(old, 1) == 1, 1.0, 0.0)
        t_ref[4 + tensor] = jnp.full((1, LANES), swapped, jnp.float32)
    for turn, target in enumerate((key0_hbm, key1_hbm)):
        key_smem[turn, 0] = 2 * rows[turn] + odds[1 - turn]
        copies.append(pltpu.make_async_copy(key_smem.at[turn], target, sems.at[3 + turn]))
        copies[-1].start()
    for number in range(3):
        for copy in copies[number : 2 * 3 : 3]:
            copy.wait()

        def pick(part, number=number):
            for tensor in range(tensors):
                s_ref[tensor, number, part, :] = jnp.where(
                    cores[tensor] == 1,
                    both[1, tensor, number, part, :],
                    both[0, tensor, number, part, :],
                )

        by_rows(length, 64, pick)
    for copy in copies[2 * 3 :]:
        copy.wait()
    swap.wait()
    t_ref[0] = sums[0] + sums[1]
    t_ref[1] = sums[0] + sums[1]


def adam_update(params, first_moment, second_moment, gradients, clip_factor):
    scaled = clip_factor * gradients
    first_new = beta_one * first_moment + (1.0 - beta_one) * scaled
    second_new = beta_two * second_moment + (1.0 - beta_two) * scaled * scaled
    bias_first = 1.0 - beta_one**STEP
    bias_second = 1.0 - beta_two**STEP
    update = first_new * (1.0 / bias_first) / (jnp.sqrt(second_new * (1.0 / bias_second)) + epsilon)
    params_new = params - learn_rate * (update + decay_rate * params)
    return (params_new, first_new, second_new)


def adam(limit, t_ref, s_ref, g_ref, po_hbm, mo_hbm, vo_hbm, po_ref, mo_ref, vo_ref, sems):
    squares = jnp.full((SUBLANES, LANES), jnp.sum(t_ref[1]), jnp.float32)
    clip = limit / jnp.maximum(jnp.sqrt(squares), limit)
    length = g_ref.shape[1]
    half = length // 2
    step = 32
    tile = (step // SUBLANES, SUBLANES, LANES)
    copies = []
    for tensor in range(2):
        crossed = jnp.broadcast_to(t_ref[4 + tensor], (SUBLANES, LANES))[None] > 0.5

        def body(i, carry, crossed=crossed, tensor=tensor):
            halves = [
                [
                    s_ref[tensor, number, pl.ds(side + 2 * i * step, step, stride=2), :].reshape(tile)
                    for number in range(3)
                ]
                for side in range(2)
            ]
            for side in range(2):
                at = pl.ds(pl.multiple_of(side * half + i * step, step), step)
                values = [
                    jnp.where(crossed, other, own)
                    for own, other in zip(halves[side], halves[1 - side])
                ]
                new = adam_update(*values, g_ref[tensor, at, :].reshape(tile), clip[None])
                for ref, value in zip((po_ref, mo_ref, vo_ref), new):
                    ref[tensor, at, :] = value.reshape(step, LANES)
            return carry

        parts = 2
        for part in range(parts):
            steps = half // step // parts
            lax.fori_loop(part * steps, (part + 1) * steps, body, 0)
            for side in range(2):
                at = pl.ds(side * half + part * steps * step, steps * step)
                for number, (source, target) in enumerate(
                    ((po_ref, po_hbm), (mo_ref, mo_hbm), (vo_ref, vo_hbm))
                ):
                    copy = pltpu.make_async_copy(
                        source.at[tensor, at],
                        target.at[tensor, at],
                        sems.at[tensor, part, side, number],
                    )
                    copy.start()
                    copies.append(copy)
    for copy in copies:
        copy.wait()


def chosen_branch(index, branches, *operands):
    traced = jax.make_jaxpr(lambda i, *xs: lax.switch(i, branches, *xs))(index, *operands)
    choice = traced.eqns[-1]
    return choice.primitive.bind(index, *operands, **choice.params)


def shards(total, old_params, old_first, old_second, gradients, old_table, new_table):
    tensors, _, width = old_params.shape
    rows = 2 * width // LANES

    def lined(x):
        x = x.reshape(tensors, 2, width // LANES, LANES)
        return x.transpose(0, 2, 1, 3).reshape(tensors, rows, LANES)

    anywhere = pl.BlockSpec(memory_space=pl.ANY)
    whole = pl.BlockSpec(memory_space=pltpu.VMEM)
    state = jax.ShapeDtypeStruct((tensors, 3, rows, LANES), jnp.float32)
    value = jax.ShapeDtypeStruct((6, 1, LANES), jnp.float32)
    key = jax.ShapeDtypeStruct((1,), jnp.int32)
    full = jax.ShapeDtypeStruct((tensors, rows, LANES), jnp.float32)
    variants = [(row_key, odd) for row_key in range(16) for odd in range(2)]
    gradients = gradients.reshape(tensors, rows, LANES)
    stacked, shared, *keys = pl.pallas_call(
        gather,
        out_shape=(state, value, key, key),
        in_specs=[anywhere] * 6,
        out_specs=[whole] * 2 + [anywhere] * 2,
        scratch_shapes=[
            pltpu.VMEM(full.shape, jnp.float32),
            pltpu.VMEM((2, *state.shape), jnp.float32),
            pltpu.SMEM((tensors, LANES), jnp.int32),
            pltpu.SMEM((tensors, LANES), jnp.int32),
            pltpu.SMEM((2, 1), jnp.int32),
            pltpu.VMEM((2, 1, LANES), jnp.float32),
            pltpu.SemaphoreType.DMA((5,)),
            pltpu.SemaphoreType.DMA((3, 3)),
            pltpu.SemaphoreType.DMA((2,)),
        ],
        compiler_params=pltpu.CompilerParams(
            collective_id=len(variants), has_side_effects=True
        ),
        name="gather",
    )(
        *(lined(x) for x in (old_params, old_first, old_second)),
        gradients,
        old_table,
        new_table,
    )
    branches = [exchanged(row_key, odd, state, value) for row_key, odd in variants]

    for key in keys:
        stacked, shared = chosen_branch(key.reshape(()), branches, stacked, shared)
    new = pl.pallas_call(
        functools.partial(adam, 0.5 * math.sqrt(gradients.size * total)),
        out_shape=(full,) * 3,
        in_specs=[whole] * 3,
        out_specs=[anywhere] * 3,
        scratch_shapes=[pltpu.VMEM(full.shape, jnp.float32)] * 3
        + [pltpu.SemaphoreType.DMA((tensors, 2, 2, 3))],
        name="adam",
    )(shared, stacked, gradients)
    return tuple(x.reshape(tensors, 1, rows * LANES) for x in new)


def solution(mesh):
    split = P(None, AXES, None)
    return jax.shard_map(
        functools.partial(shards, mesh.size),
        mesh=mesh,
        in_specs=(split,) * 4 + (P(), P()),
        out_specs=(split,) * 3,
        check_vma=False,
    )
```

```python
import functools
import math

import jax
import jax.numpy as jnp
from jax import lax
from jax.experimental import pallas as pl
from jax.experimental.pallas import tpu as pltpu
from jax.sharding import PartitionSpec as P

STEP = 100
MESH = pl.DeviceIdType.MESH
AXES = ("row", "col")
LANES = 128
SUBLANES = 8

beta_one = 0.9
beta_two = 0.95
epsilon = 1e-08
learn_rate = 0.001
decay_rate = 0.1

STAGE = 7


def stage_masks(member, far):
    scale = 3 if far else 1
    return (((member & 1) * 4 + ((member >> 1) & 1)) * scale, (member >> 2) * 2 * scale)


def flip(index, bits):
    return jnp.bitwise_xor(index, bits)


def by_rows(rows, step, move):
    def body(i, carry):
        move(pl.ds(pl.multiple_of(i * step, step), step))
        return carry

    lax.fori_loop(0, rows // step, body, 0)


def exchange(
    row_key, odd, s_ref, v_ref, o_ref, t_ref, landed, slots, go, here, ready, small, tell, bulk, sides
):
    row, col = lax.axis_index("row"), lax.axis_index("col")
    planes, rows, _ = s_ref.shape[1:]
    core = col % 2
    twin = (row, flip(col, 1))
    barrier = pltpu.get_barrier_semaphore()
    sides_of = (((0, 2), 0), ((0, 6), 1)) if odd else (((0, 4), 1),)
    partners = [mask for mask, _ in sides_of]
    if row_key:
        partners.append((row_key, 0))

    def at(mask):
        return (flip(row, mask[0]), flip(col, mask[1]))

    @pl.when(core == 1)
    def _():
        for mask in partners:
            pl.semaphore_signal(barrier, inc=1, device_id=at(mask), device_id_type=MESH)
        pl.semaphore_signal(barrier, inc=1, device_id=twin, device_id_type=MESH)
        pl.semaphore_wait(barrier, len(partners))

    @pl.when(core == 0)
    def _():
        def greet(member, carry):
            for far in range(2):
                peer = at(stage_masks(member, far))
                pl.semaphore_signal(barrier, inc=1, device_id=peer, device_id_type=MESH)
            return carry

        lax.fori_loop(1, STAGE + 1, greet, 0)
        pl.semaphore_wait(barrier, 2 * STAGE + 1)
        pl.semaphore_signal(here, inc=1, device_id=twin, device_id_type=MESH)

        def give(member, carry):
            for far in range(2):
                pltpu.make_async_remote_copy(
                    src_ref=v_ref.at[0],
                    dst_ref=slots.at[far, member - 1],
                    send_sem=small.at[0],
                    recv_sem=small.at[1],
                    device_id=at(stage_masks(member, far)),
                    device_id_type=MESH,
                ).start()
            return carry

        lax.fori_loop(1, STAGE + 1, give, 0)
        pl.semaphore_wait(go, 1)

    streams = []
    if row_key:
        streams.append((0, o_ref.at[1], bulk, (row_key, 0)))
    for mask, place in sides_of:
        streams.append((1, landed.at[place], sides.at[place], mask))
    copies = [
        [
            pltpu.make_async_remote_copy(
                src_ref=s_ref.at[tensor, plane],
                dst_ref=target.at[plane],
                send_sem=sems.at[0, plane],
                recv_sem=sems.at[1, plane],
                device_id=at(mask),
                device_id_type=MESH,
            )
            for tensor, target, sems, mask in streams
        ]
        for plane in range(planes)
    ]
    for plane in copies:
        for copy in plane:
            copy.start()

    @pl.when(core == 1)
    def _():
        pl.semaphore_wait(here, 1)
        for mask in partners:
            pl.semaphore_signal(ready, inc=1, device_id=at(mask), device_id_type=MESH)
        pl.semaphore_wait(ready, len(partners))
        pl.semaphore_signal(go, inc=1, device_id=twin, device_id_type=MESH)

    if not row_key:

        def keep(part):
            for plane in range(planes):
                o_ref[1, plane, part, :] = s_ref[0, plane, part, :]

        by_rows(rows, 64, keep)
    forward = pltpu.make_async_remote_copy(
        src_ref=slots,
        dst_ref=slots,
        send_sem=tell.at[0],
        recv_sem=tell.at[1],
        device_id=twin,
        device_id_type=MESH,
    )

    @pl.when(core == 0)
    def _():
        pltpu.make_async_remote_copy(
            src_ref=slots,
            dst_ref=slots,
            send_sem=small.at[0],
            recv_sem=small.at[1],
            device_id=twin,
            device_id_type=MESH,
        ).wait()
        forward.start()
        forward.wait_send()

    @pl.when(core == 1)
    def _():
        forward.wait_recv()

    t_ref[0:2] = v_ref[0][None] + jnp.sum(slots[...], axis=1)
    t_ref[2] = v_ref[3]
    t_ref[3] = v_ref[2]
    t_ref[4:6] = v_ref[4:6]
    chosen = v_ref[2] > 0.5
    across = 1 if row_key else 0
    for plane in range(planes):
        for copy in copies[plane][across:]:
            copy.wait_recv()

        def pick(part, plane=plane):
            other = landed[0, plane, part, :] if odd else s_ref[1, plane, part, :]
            o_ref[0, plane, part, :] = jnp.where(chosen, landed[1, plane, part, :], other)

        by_rows(rows, 128, pick)
    for plane in copies:
        for copy in plane[:across]:
            copy.wait_recv()
    for plane in copies:
        for copy in plane:
            copy.wait_send()


def exchanged(row_key, odd, state, value):
    whole = pl.BlockSpec(memory_space=pltpu.VMEM)
    return pl.pallas_call(
        functools.partial(exchange, row_key, odd),
        out_shape=(state, value),
        in_specs=[whole] * 2,
        out_specs=[whole] * 2,
        scratch_shapes=[
            pltpu.VMEM(state.shape, jnp.float32),
            pltpu.VMEM((2, STAGE, 1, LANES), jnp.float32),
            pltpu.SemaphoreType.REGULAR,
            pltpu.SemaphoreType.REGULAR,
            pltpu.SemaphoreType.REGULAR,
            pltpu.SemaphoreType.DMA((2,)),
            pltpu.SemaphoreType.DMA((2,)),
            pltpu.SemaphoreType.DMA((2, 3)),
            pltpu.SemaphoreType.DMA((2, 2, 3)),
        ],
        compiler_params=pltpu.CompilerParams(
            collective_id=2 * row_key + odd, has_side_effects=True
        ),
        name="exchange",
    )


def gather(
    p_ref, m_ref, v_ref, g_hbm, old_hbm, new_hbm,
    s_ref, t_ref, key0_hbm, key1_hbm,
    g_ref, both, old_smem, new_smem, key_smem, sums, sems, state_sems, core_sems,
):
    row, col = lax.axis_index("row"), lax.axis_index("col")
    twin = (row, flip(col, 1))
    barrier = pltpu.get_barrier_semaphore()
    pl.semaphore_signal(barrier, inc=1, device_id=twin, device_id_type=MESH)
    smalls = [
        pltpu.make_async_copy(old_hbm.at[:, pl.ds(0, LANES)], old_smem, sems.at[0]),
        pltpu.make_async_copy(new_hbm.at[:, pl.ds(0, LANES)], new_smem, sems.at[1]),
    ]
    gradient = pltpu.make_async_copy(g_hbm, g_ref, sems.at[2])
    gradient.start()
    for copy in smalls:
        copy.start()
    copies = []
    for number, source in enumerate((p_ref, m_ref, v_ref)):
        copies.append(
            pltpu.make_async_copy(source, both.at[0, :, number], state_sems.at[0, number])
        )
        copies[-1].start()
    pl.semaphore_wait(barrier, 1)
    for number, source in enumerate((p_ref, m_ref, v_ref)):
        copies.append(
            pltpu.make_async_remote_copy(
                src_ref=source,
                dst_ref=both.at[1, :, number],
                send_sem=state_sems.at[1, number],
                recv_sem=state_sems.at[2, number],
                device_id=twin,
                device_id_type=MESH,
            )
        )
        copies[-1].start()
    gradient.wait()
    tensors, length, _ = g_ref.shape
    step = 64

    def body(i, total):
        at = pl.ds(pl.multiple_of(i * step, step), step)
        for tensor in range(tensors):
            g = g_ref[tensor, at, :].reshape(step // SUBLANES, SUBLANES, LANES)
            total = total + jnp.sum(g * g, axis=0)
        return total

    total = lax.fori_loop(0, length // step, body, jnp.zeros((SUBLANES, LANES), jnp.float32))
    sums[0] = jnp.sum(total, axis=0, keepdims=True)
    swap = pltpu.make_async_remote_copy(
        src_ref=sums.at[0],
        dst_ref=sums.at[1],
        send_sem=core_sems.at[0],
        recv_sem=core_sems.at[1],
        device_id=twin,
        device_id_type=MESH,
    )
    swap.start()
    for copy in smalls:
        copy.wait()
    rows, odds, cores = [], [], []
    for tensor in range(2):
        old = old_smem[tensor, 0]
        route = jnp.bitwise_xor(jnp.right_shift(old, 1), new_smem[tensor, 0])
        key_y = jnp.bitwise_and(jnp.right_shift(route, 1), 3)
        odd = jnp.bitwise_and(key_y, 1)
        second = jnp.where(key_y >= 2, 1.0, 0.0)
        rows.append(jnp.right_shift(route, 3))
        odds.append(odd)
        cores.append(jnp.bitwise_and(route, 1))
        t_ref[3 - tensor] = jnp.full((1, LANES), second, jnp.float32)
        swapped = jnp.where(jnp.bitwise_and(old, 1) == 1, 1.0, 0.0)
        t_ref[4 + tensor] = jnp.full((1, LANES), swapped, jnp.float32)
    for turn, target in enumerate((key0_hbm, key1_hbm)):
        key_smem[turn, 0] = 2 * rows[turn] + odds[1 - turn]
        copies.append(pltpu.make_async_copy(key_smem.at[turn], target, sems.at[3 + turn]))
        copies[-1].start()
    for number in range(3):
        for copy in copies[number : 2 * 3 : 3]:
            copy.wait()

        def pick(part, number=number):
            for tensor in range(tensors):
                s_ref[tensor, number, part, :] = jnp.where(
                    cores[tensor] == 1,
                    both[1, tensor, number, part, :],
                    both[0, tensor, number, part, :],
                )

        by_rows(length, 64, pick)
    for copy in copies[2 * 3 :]:
        copy.wait()
    swap.wait()
    t_ref[0] = sums[0] + sums[1]
    t_ref[1] = sums[0] + sums[1]


def adam_update(params, first_moment, second_moment, gradients, clip_factor):
    scaled = clip_factor * gradients
    first_new = beta_one * first_moment + (1.0 - beta_one) * scaled
    second_new = beta_two * second_moment + (1.0 - beta_two) * scaled * scaled
    bias_first = 1.0 - beta_one**STEP
    bias_second = 1.0 - beta_two**STEP
    update = first_new * (1.0 / bias_first) / (jnp.sqrt(second_new * (1.0 / bias_second)) + epsilon)
    params_new = params - learn_rate * (update + decay_rate * params)
    return (params_new, first_new, second_new)


def adam(limit, t_ref, s_ref, g_hbm, po_hbm, mo_hbm, vo_hbm, po_ref, mo_ref, vo_ref, g_ref, sems, loads):
    gradient = [
        pltpu.make_async_copy(g_hbm.at[tensor], g_ref.at[tensor], loads.at[tensor])
        for tensor in range(2)
    ]
    for copy in gradient:
        copy.start()
    squares = jnp.full((SUBLANES, LANES), jnp.sum(t_ref[1]), jnp.float32)
    clip = limit / jnp.maximum(jnp.sqrt(squares), limit)
    length = s_ref.shape[2]
    half = length // 2
    step = 64
    tile = (step // SUBLANES, SUBLANES, LANES)
    outputs = ((po_ref, po_hbm), (mo_ref, mo_hbm), (vo_ref, vo_hbm))
    for tensor in range(2):
        crossed = jnp.broadcast_to(t_ref[4 + tensor], (step, LANES)) > 0.5

        def lay(i, carry, crossed=crossed, tensor=tensor):
            for number, (ref, _) in enumerate(outputs):
                even, odd = (
                    s_ref[tensor, number, pl.ds(side + 2 * i * step, step, stride=2), :]
                    for side in range(2)
                )
                for side, value in enumerate(
                    (jnp.where(crossed, odd, even), jnp.where(crossed, even, odd))
                ):
                    at = pl.ds(pl.multiple_of(side * half + i * step, step), step)
                    ref[tensor, at, :] = value
            return carry

        lax.fori_loop(0, half // step, lay, 0)
    copies = []
    parts = 4
    for tensor in range(2):
        gradient[tensor].wait()

        def update(i, carry, tensor=tensor):
            at = pl.ds(pl.multiple_of(i * step, step), step)
            values = [ref[tensor, at, :].reshape(tile) for ref in (po_ref, mo_ref, vo_ref, g_ref)]
            for (ref, _), value in zip(outputs, adam_update(*values, clip[None])):
                ref[tensor, at, :] = value.reshape(step, LANES)
            return carry

        for part in range(parts):
            steps = length // step // parts
            lax.fori_loop(part * steps, (part + 1) * steps, update, 0)
            at = pl.ds(part * steps * step, steps * step)
            for number, (source, target) in enumerate(outputs):
                copy = pltpu.make_async_copy(
                    source.at[tensor, at], target.at[tensor, at], sems.at[tensor, part, number]
                )
                copy.start()
                copies.append(copy)
    for copy in copies:
        copy.wait()


def chosen_branch(index, branches, *operands):
    traced = jax.make_jaxpr(lambda i, *xs: lax.switch(i, branches, *xs))(index, *operands)
    choice = traced.eqns[-1]
    return choice.primitive.bind(index, *operands, **choice.params)


def shards(total, old_params, old_first, old_second, gradients, old_table, new_table):
    tensors, _, width = old_params.shape
    rows = 2 * width // LANES

    def lined(x):
        x = x.reshape(tensors, 2, width // LANES, LANES)
        return x.transpose(0, 2, 1, 3).reshape(tensors, rows, LANES)

    anywhere = pl.BlockSpec(memory_space=pl.ANY)
    whole = pl.BlockSpec(memory_space=pltpu.VMEM)
    state = jax.ShapeDtypeStruct((tensors, 3, rows, LANES), jnp.float32)
    value = jax.ShapeDtypeStruct((6, 1, LANES), jnp.float32)
    key = jax.ShapeDtypeStruct((1,), jnp.int32)
    full = jax.ShapeDtypeStruct((tensors, rows, LANES), jnp.float32)
    variants = [(row_key, odd) for row_key in range(16) for odd in range(2)]
    gradients = gradients.reshape(tensors, rows, LANES)
    stacked, shared, *keys = pl.pallas_call(
        gather,
        out_shape=(state, value, key, key),
        in_specs=[anywhere] * 6,
        out_specs=[whole] * 2 + [anywhere] * 2,
        scratch_shapes=[
            pltpu.VMEM(full.shape, jnp.float32),
            pltpu.VMEM((2, *state.shape), jnp.float32),
            pltpu.SMEM((tensors, LANES), jnp.int32),
            pltpu.SMEM((tensors, LANES), jnp.int32),
            pltpu.SMEM((2, 1), jnp.int32),
            pltpu.VMEM((2, 1, LANES), jnp.float32),
            pltpu.SemaphoreType.DMA((5,)),
            pltpu.SemaphoreType.DMA((3, 3)),
            pltpu.SemaphoreType.DMA((2,)),
        ],
        compiler_params=pltpu.CompilerParams(
            collective_id=len(variants), has_side_effects=True
        ),
        name="gather",
    )(
        *(lined(x) for x in (old_params, old_first, old_second)),
        gradients,
        old_table,
        new_table,
    )
    branches = [exchanged(row_key, odd, state, value) for row_key, odd in variants]

    for key in keys:
        stacked, shared = chosen_branch(key.reshape(()), branches, stacked, shared)
    new = pl.pallas_call(
        functools.partial(adam, 0.5 * math.sqrt(gradients.size * total)),
        out_shape=(full,) * 3,
        in_specs=[whole] * 2 + [anywhere],
        out_specs=[anywhere] * 3,
        scratch_shapes=[pltpu.VMEM(full.shape, jnp.float32)] * 4
        + [pltpu.SemaphoreType.DMA((tensors, 4, 3)), pltpu.SemaphoreType.DMA((tensors,))],
        name="adam",
    )(shared, stacked, gradients)
    return tuple(x.reshape(tensors, 1, rows * LANES) for x in new)


def solution(mesh):
    split = P(None, AXES, None)
    return jax.shard_map(
        functools.partial(shards, mesh.size),
        mesh=mesh,
        in_specs=(split,) * 4 + (P(), P()),
        out_specs=(split,) * 3,
        check_vma=False,
    )
```

```python
import functools
import math

import jax
import jax.numpy as jnp
from jax import lax
from jax.experimental import pallas as pl
from jax.experimental.pallas import tpu as pltpu
from jax.sharding import PartitionSpec as P

STEP = 100
MESH = pl.DeviceIdType.MESH
AXES = ("row", "col")
LANES = 128
SUBLANES = 8

beta_one = 0.9
beta_two = 0.95
epsilon = 1e-08
learn_rate = 0.001
decay_rate = 0.1

STAGE = 7


def stage_masks(member, far):
    scale = 3 if far else 1
    return (((member & 1) * 4 + ((member >> 1) & 1)) * scale, (member >> 2) * 2 * scale)


def flip(index, bits):
    return jnp.bitwise_xor(index, bits)


def by_rows(rows, step, move):
    def body(i, carry):
        move(pl.ds(pl.multiple_of(i * step, step), step))
        return carry

    lax.fori_loop(0, rows // step, body, 0)


def exchange(
    row_key, odd, s_ref, v_ref, o_ref, t_ref, landed, slots, go, here, ready, small, tell, bulk, sides
):
    row, col = lax.axis_index("row"), lax.axis_index("col")
    planes, rows, _ = s_ref.shape[1:]
    core = col % 2
    twin = (row, flip(col, 1))
    barrier = pltpu.get_barrier_semaphore()
    sides_of = (((0, 2), 0), ((0, 6), 1)) if odd else (((0, 4), 1),)
    partners = [mask for mask, _ in sides_of]
    if row_key:
        partners.append((row_key, 0))

    def at(mask):
        return (flip(row, mask[0]), flip(col, mask[1]))

    @pl.when(core == 1)
    def _():
        for mask in partners:
            pl.semaphore_signal(barrier, inc=1, device_id=at(mask), device_id_type=MESH)
        pl.semaphore_signal(barrier, inc=1, device_id=twin, device_id_type=MESH)
        pl.semaphore_wait(barrier, len(partners))

    @pl.when(core == 0)
    def _():
        def greet(member, carry):
            for far in range(2):
                peer = at(stage_masks(member, far))
                pl.semaphore_signal(barrier, inc=1, device_id=peer, device_id_type=MESH)
            return carry

        lax.fori_loop(1, STAGE + 1, greet, 0)
        pl.semaphore_wait(barrier, 2 * STAGE + 1)
        pl.semaphore_signal(here, inc=1, device_id=twin, device_id_type=MESH)

        def give(member, carry):
            for far in range(2):
                pltpu.make_async_remote_copy(
                    src_ref=v_ref.at[0],
                    dst_ref=slots.at[far, member - 1],
                    send_sem=small.at[0],
                    recv_sem=small.at[1],
                    device_id=at(stage_masks(member, far)),
                    device_id_type=MESH,
                ).start()
            return carry

        lax.fori_loop(1, STAGE + 1, give, 0)
        pl.semaphore_wait(go, 1)

    streams = []
    if row_key:
        streams.append((0, o_ref.at[1], bulk, (row_key, 0)))
    for mask, place in sides_of:
        streams.append((1, landed.at[place], sides.at[place], mask))
    copies = [
        [
            pltpu.make_async_remote_copy(
                src_ref=s_ref.at[tensor, plane],
                dst_ref=target.at[plane],
                send_sem=sems.at[0, plane],
                recv_sem=sems.at[1, plane],
                device_id=at(mask),
                device_id_type=MESH,
            )
            for tensor, target, sems, mask in streams
        ]
        for plane in range(planes)
    ]
    for plane in copies:
        for copy in plane:
            copy.start()

    @pl.when(core == 1)
    def _():
        pl.semaphore_wait(here, 1)
        for mask in partners:
            pl.semaphore_signal(ready, inc=1, device_id=at(mask), device_id_type=MESH)
        pl.semaphore_wait(ready, len(partners))
        pl.semaphore_signal(go, inc=1, device_id=twin, device_id_type=MESH)

    if not row_key:

        def keep(part):
            for plane in range(planes):
                o_ref[1, plane, part, :] = s_ref[0, plane, part, :]

        by_rows(rows, 64, keep)
    forward = pltpu.make_async_remote_copy(
        src_ref=slots,
        dst_ref=slots,
        send_sem=tell.at[0],
        recv_sem=tell.at[1],
        device_id=twin,
        device_id_type=MESH,
    )

    @pl.when(core == 0)
    def _():
        pltpu.make_async_remote_copy(
            src_ref=slots,
            dst_ref=slots,
            send_sem=small.at[0],
            recv_sem=small.at[1],
            device_id=twin,
            device_id_type=MESH,
        ).wait()
        forward.start()
        forward.wait_send()

    @pl.when(core == 1)
    def _():
        forward.wait_recv()

    t_ref[0:2] = v_ref[0][None] + jnp.sum(slots[...], axis=1)
    t_ref[2] = v_ref[3]
    t_ref[3] = v_ref[2]
    t_ref[4:6] = v_ref[4:6]
    chosen = v_ref[2] > 0.5
    across = 1 if row_key else 0
    for plane in range(planes):
        for copy in copies[plane][across:]:
            copy.wait_recv()

        def pick(part, plane=plane):
            other = landed[0, plane, part, :] if odd else s_ref[1, plane, part, :]
            o_ref[0, plane, part, :] = jnp.where(chosen, landed[1, plane, part, :], other)

        by_rows(rows, 128, pick)
    for plane in copies:
        for copy in plane[:across]:
            copy.wait_recv()
    for plane in copies:
        for copy in plane:
            copy.wait_send()


def exchanged(row_key, odd, state, value):
    whole = pl.BlockSpec(memory_space=pltpu.VMEM)
    return pl.pallas_call(
        functools.partial(exchange, row_key, odd),
        out_shape=(state, value),
        in_specs=[whole] * 2,
        out_specs=[whole] * 2,
        scratch_shapes=[
            pltpu.VMEM(state.shape, jnp.float32),
            pltpu.VMEM((2, STAGE, 1, LANES), jnp.float32),
            pltpu.SemaphoreType.REGULAR,
            pltpu.SemaphoreType.REGULAR,
            pltpu.SemaphoreType.REGULAR,
            pltpu.SemaphoreType.DMA((2,)),
            pltpu.SemaphoreType.DMA((2,)),
            pltpu.SemaphoreType.DMA((2, 3)),
            pltpu.SemaphoreType.DMA((2, 2, 3)),
        ],
        compiler_params=pltpu.CompilerParams(
            collective_id=2 * row_key + odd, has_side_effects=True
        ),
        name="exchange",
    )


def gather(
    p_ref, m_ref, v_ref, g_hbm, old_hbm, new_hbm,
    s_ref, t_ref, key0_hbm, key1_hbm,
    g_ref, both, old_smem, new_smem, key_smem, sums, sems, state_sems, core_sems,
):
    row, col = lax.axis_index("row"), lax.axis_index("col")
    twin = (row, flip(col, 1))
    barrier = pltpu.get_barrier_semaphore()
    pl.semaphore_signal(barrier, inc=1, device_id=twin, device_id_type=MESH)
    smalls = [
        pltpu.make_async_copy(old_hbm.at[:, pl.ds(0, LANES)], old_smem, sems.at[0]),
        pltpu.make_async_copy(new_hbm.at[:, pl.ds(0, LANES)], new_smem, sems.at[1]),
    ]
    gradient = pltpu.make_async_copy(g_hbm, g_ref, sems.at[2])
    gradient.start()
    for copy in smalls:
        copy.start()
    copies = []
    for number, source in enumerate((p_ref, m_ref, v_ref)):
        copies.append(
            pltpu.make_async_copy(source, both.at[0, :, number], state_sems.at[0, number])
        )
        copies[-1].start()
    pl.semaphore_wait(barrier, 1)
    for number, source in enumerate((p_ref, m_ref, v_ref)):
        copies.append(
            pltpu.make_async_remote_copy(
                src_ref=source,
                dst_ref=both.at[1, :, number],
                send_sem=state_sems.at[1, number],
                recv_sem=state_sems.at[2, number],
                device_id=twin,
                device_id_type=MESH,
            )
        )
        copies[-1].start()
    gradient.wait()
    tensors, length, _ = g_ref.shape
    step = 64

    def body(i, total):
        at = pl.ds(pl.multiple_of(i * step, step), step)
        for tensor in range(tensors):
            g = g_ref[tensor, at, :].reshape(step // SUBLANES, SUBLANES, LANES)
            total = total + jnp.sum(g * g, axis=0)
        return total

    total = lax.fori_loop(0, length // step, body, jnp.zeros((SUBLANES, LANES), jnp.float32))
    sums[0] = jnp.sum(total, axis=0, keepdims=True)
    for copy in smalls:
        copy.wait()
    rows, odds, cores = [], [], []
    for tensor in range(2):
        old = old_smem[tensor, 0]
        route = jnp.bitwise_xor(jnp.right_shift(old, 1), new_smem[tensor, 0])
        key_y = jnp.bitwise_and(jnp.right_shift(route, 1), 3)
        odd = jnp.bitwise_and(key_y, 1)
        second = jnp.where(key_y >= 2, 1.0, 0.0)
        rows.append(jnp.right_shift(route, 3))
        odds.append(odd)
        cores.append(jnp.bitwise_and(route, 1))
        t_ref[3 - tensor] = jnp.full((1, LANES), second, jnp.float32)
        swapped = jnp.where(jnp.bitwise_and(old, 1) == 1, 1.0, 0.0)
        t_ref[4 + tensor] = jnp.full((1, LANES), swapped, jnp.float32)
    keys = []
    for turn, target in enumerate((key0_hbm, key1_hbm)):
        key_smem[turn, 0] = 2 * rows[turn] + odds[1 - turn]
        keys.append(pltpu.make_async_copy(key_smem.at[turn], target, sems.at[3 + turn]))
    swap = pltpu.make_async_remote_copy(
        src_ref=sums.at[0],
        dst_ref=sums.at[1],
        send_sem=core_sems.at[0],
        recv_sem=core_sems.at[1],
        device_id=twin,
        device_id_type=MESH,
    )
    swap.start()
    for number in range(3):
        for copy in copies[number::3]:
            copy.wait()
        if number == 0:
            for copy in keys:
                copy.start()

        def pick(part, number=number):
            for tensor in range(tensors):
                s_ref[tensor, number, part, :] = jnp.where(
                    cores[tensor] == 1,
                    both[1, tensor, number, part, :],
                    both[0, tensor, number, part, :],
                )

        by_rows(length, 64, pick)
    for copy in keys:
        copy.wait()
    swap.wait()
    t_ref[0] = sums[0] + sums[1]
    t_ref[1] = sums[0] + sums[1]


def adam_update(params, first_moment, second_moment, gradients, clip_factor):
    scaled = clip_factor * gradients
    first_new = beta_one * first_moment + (1.0 - beta_one) * scaled
    second_new = beta_two * second_moment + (1.0 - beta_two) * scaled * scaled
    bias_first = 1.0 - beta_one**STEP
    bias_second = 1.0 - beta_two**STEP
    update = first_new * (1.0 / bias_first) / (jnp.sqrt(second_new * (1.0 / bias_second)) + epsilon)
    params_new = params - learn_rate * (update + decay_rate * params)
    return (params_new, first_new, second_new)


def adam(limit, t_ref, s_ref, g_hbm, po_hbm, mo_hbm, vo_hbm, po_ref, mo_ref, vo_ref, g_ref, sems, loads):
    gradient = [
        pltpu.make_async_copy(g_hbm.at[tensor], g_ref.at[tensor], loads.at[tensor])
        for tensor in range(2)
    ]
    for copy in gradient:
        copy.start()
    squares = jnp.full((SUBLANES, LANES), jnp.sum(t_ref[1]), jnp.float32)
    clip = limit / jnp.maximum(jnp.sqrt(squares), limit)
    length = s_ref.shape[2]
    half = length // 2
    step = 64
    tile = (step // SUBLANES, SUBLANES, LANES)
    outputs = ((po_ref, po_hbm), (mo_ref, mo_hbm), (vo_ref, vo_hbm))
    for tensor in range(2):
        crossed = jnp.broadcast_to(t_ref[4 + tensor], (step, LANES)) > 0.5

        def lay(i, carry, crossed=crossed, tensor=tensor):
            for number, (ref, _) in enumerate(outputs):
                even, odd = (
                    s_ref[tensor, number, pl.ds(side + 2 * i * step, step, stride=2), :]
                    for side in range(2)
                )
                for side, value in enumerate(
                    (jnp.where(crossed, odd, even), jnp.where(crossed, even, odd))
                ):
                    at = pl.ds(pl.multiple_of(side * half + i * step, step), step)
                    ref[tensor, at, :] = value
            return carry

        lax.fori_loop(0, half // step, lay, 0)
    copies = []
    parts = 4
    for tensor in range(2):
        gradient[tensor].wait()

        def update(i, carry, tensor=tensor):
            at = pl.ds(pl.multiple_of(i * step, step), step)
            values = [ref[tensor, at, :].reshape(tile) for ref in (po_ref, mo_ref, vo_ref, g_ref)]
            for (ref, _), value in zip(outputs, adam_update(*values, clip[None])):
                ref[tensor, at, :] = value.reshape(step, LANES)
            return carry

        for part in range(parts):
            steps = length // step // parts
            lax.fori_loop(part * steps, (part + 1) * steps, update, 0)
            at = pl.ds(part * steps * step, steps * step)
            for number, (source, target) in enumerate(outputs):
                copy = pltpu.make_async_copy(
                    source.at[tensor, at], target.at[tensor, at], sems.at[tensor, part, number]
                )
                copy.start()
                copies.append(copy)
    for copy in copies:
        copy.wait()


def chosen_branch(index, branches, *operands):
    traced = jax.make_jaxpr(lambda i, *xs: lax.switch(i, branches, *xs))(index, *operands)
    choice = traced.eqns[-1]
    return choice.primitive.bind(index, *operands, **choice.params)


def shards(total, old_params, old_first, old_second, gradients, old_table, new_table):
    tensors, _, width = old_params.shape
    rows = 2 * width // LANES

    def lined(x):
        x = x.reshape(tensors, 2, width // LANES, LANES)
        return x.transpose(0, 2, 1, 3).reshape(tensors, rows, LANES)

    anywhere = pl.BlockSpec(memory_space=pl.ANY)
    whole = pl.BlockSpec(memory_space=pltpu.VMEM)
    state = jax.ShapeDtypeStruct((tensors, 3, rows, LANES), jnp.float32)
    value = jax.ShapeDtypeStruct((6, 1, LANES), jnp.float32)
    key = jax.ShapeDtypeStruct((1,), jnp.int32)
    full = jax.ShapeDtypeStruct((tensors, rows, LANES), jnp.float32)
    variants = [(row_key, odd) for row_key in range(16) for odd in range(2)]
    gradients = gradients.reshape(tensors, rows, LANES)
    stacked, shared, *keys = pl.pallas_call(
        gather,
        out_shape=(state, value, key, key),
        in_specs=[anywhere] * 6,
        out_specs=[whole] * 2 + [anywhere] * 2,
        scratch_shapes=[
            pltpu.VMEM(full.shape, jnp.float32),
            pltpu.VMEM((2, *state.shape), jnp.float32),
            pltpu.SMEM((tensors, LANES), jnp.int32),
            pltpu.SMEM((tensors, LANES), jnp.int32),
            pltpu.SMEM((2, 1), jnp.int32),
            pltpu.VMEM((2, 1, LANES), jnp.float32),
            pltpu.SemaphoreType.DMA((5,)),
            pltpu.SemaphoreType.DMA((3, 3)),
            pltpu.SemaphoreType.DMA((2,)),
        ],
        compiler_params=pltpu.CompilerParams(
            collective_id=len(variants), has_side_effects=True
        ),
        name="gather",
    )(
        *(lined(x) for x in (old_params, old_first, old_second)),
        gradients,
        old_table,
        new_table,
    )
    branches = [exchanged(row_key, odd, state, value) for row_key, odd in variants]

    for key in keys:
        stacked, shared = chosen_branch(key.reshape(()), branches, stacked, shared)
    new = pl.pallas_call(
        functools.partial(adam, 0.5 * math.sqrt(gradients.size * total)),
        out_shape=(full,) * 3,
        in_specs=[whole] * 2 + [anywhere],
        out_specs=[anywhere] * 3,
        scratch_shapes=[pltpu.VMEM(full.shape, jnp.float32)] * 4
        + [pltpu.SemaphoreType.DMA((tensors, 4, 3)), pltpu.SemaphoreType.DMA((tensors,))],
        name="adam",
    )(shared, stacked, gradients)
    return tuple(x.reshape(tensors, 1, rows * LANES) for x in new)


def solution(mesh):
    split = P(None, AXES, None)
    return jax.shard_map(
        functools.partial(shards, mesh.size),
        mesh=mesh,
        in_specs=(split,) * 4 + (P(), P()),
        out_specs=(split,) * 3,
        check_vma=False,
    )
```

```python
import functools
import math

import jax
import jax.numpy as jnp
from jax import lax
from jax.experimental import pallas as pl
from jax.experimental.pallas import tpu as pltpu
from jax.sharding import PartitionSpec as P

STEP = 100
MESH = pl.DeviceIdType.MESH
AXES = ("row", "col")
LANES = 128
SUBLANES = 8

beta_one = 0.9
beta_two = 0.95
epsilon = 1e-08
learn_rate = 0.001
decay_rate = 0.1

STAGE = 7


def stage_masks(member, far):
    scale = 3 if far else 1
    return (((member & 1) * 4 + ((member >> 1) & 1)) * scale, (member >> 2) * 2 * scale)


def flip(index, bits):
    return jnp.bitwise_xor(index, bits)


def by_rows(rows, step, move):
    def body(i, carry):
        move(pl.ds(pl.multiple_of(i * step, step), step))
        return carry

    lax.fori_loop(0, rows // step, body, 0)


def exchange(
    row_key, odd, s_ref, v_ref, o_ref, t_ref, landed, slots, go, here, ready, small, tell, bulk, sides
):
    row, col = lax.axis_index("row"), lax.axis_index("col")
    planes, rows, _ = s_ref.shape[1:]
    core = col % 2
    twin = (row, flip(col, 1))
    barrier = pltpu.get_barrier_semaphore()
    sides_of = (((0, 2), 0), ((0, 6), 1)) if odd else (((0, 4), 1),)
    partners = [(row_key, 0)] if row_key else []
    partners += [mask for mask, _ in sides_of]

    def at(mask):
        return (flip(row, mask[0]), flip(col, mask[1]))

    @pl.when(core == 1)
    def _():
        for mask in partners:
            pl.semaphore_signal(barrier, inc=1, device_id=at(mask), device_id_type=MESH)
        pl.semaphore_signal(barrier, inc=1, device_id=twin, device_id_type=MESH)
        pl.semaphore_wait(barrier, len(partners))

    @pl.when(core == 0)
    def _():
        def greet(member, carry):
            for far in range(2):
                peer = at(stage_masks(member, far))
                pl.semaphore_signal(barrier, inc=1, device_id=peer, device_id_type=MESH)
            return carry

        lax.fori_loop(1, STAGE + 1, greet, 0)
        pl.semaphore_wait(barrier, 2 * STAGE + 1)
        pl.semaphore_signal(here, inc=1, device_id=twin, device_id_type=MESH)

        def give(member, carry):
            for far in range(2):
                pltpu.make_async_remote_copy(
                    src_ref=v_ref.at[0],
                    dst_ref=slots.at[far, member - 1],
                    send_sem=small.at[0],
                    recv_sem=small.at[1],
                    device_id=at(stage_masks(member, far)),
                    device_id_type=MESH,
                ).start()
            return carry

        lax.fori_loop(1, STAGE + 1, give, 0)
        pl.semaphore_wait(go, 1)

    streams = []
    if row_key:
        streams.append((0, o_ref.at[1], bulk, (row_key, 0)))
    for mask, place in sides_of:
        streams.append((1, landed.at[place], sides.at[place], mask))
    copies = [
        [
            pltpu.make_async_remote_copy(
                src_ref=s_ref.at[tensor, plane],
                dst_ref=target.at[plane],
                send_sem=sems.at[0, plane],
                recv_sem=sems.at[1, plane],
                device_id=at(mask),
                device_id_type=MESH,
            )
            for tensor, target, sems, mask in streams
        ]
        for plane in range(planes)
    ]
    for plane in copies:
        for copy in plane:
            copy.start()

    @pl.when(core == 1)
    def _():
        pl.semaphore_wait(here, 1)
        for mask in partners:
            pl.semaphore_signal(ready, inc=1, device_id=at(mask), device_id_type=MESH)
        pl.semaphore_wait(ready, len(partners))
        pl.semaphore_signal(go, inc=1, device_id=twin, device_id_type=MESH)

    if not row_key:

        def keep(part):
            for plane in range(planes):
                o_ref[1, plane, part, :] = s_ref[0, plane, part, :]

        by_rows(rows, 64, keep)
    forward = pltpu.make_async_remote_copy(
        src_ref=slots,
        dst_ref=slots,
        send_sem=tell.at[0],
        recv_sem=tell.at[1],
        device_id=twin,
        device_id_type=MESH,
    )

    @pl.when(core == 0)
    def _():
        pltpu.make_async_remote_copy(
            src_ref=slots,
            dst_ref=slots,
            send_sem=small.at[0],
            recv_sem=small.at[1],
            device_id=twin,
            device_id_type=MESH,
        ).wait()
        forward.start()
        forward.wait_send()

    @pl.when(core == 1)
    def _():
        forward.wait_recv()

    t_ref[0:2] = v_ref[0][None] + jnp.sum(slots[...], axis=1)
    t_ref[2] = v_ref[3]
    t_ref[3] = v_ref[2]
    t_ref[4:6] = v_ref[4:6]
    chosen = v_ref[2] > 0.5
    across = 1 if row_key else 0
    for plane in range(planes):
        for copy in copies[plane][across:]:
            copy.wait_recv()

        def pick(part, plane=plane):
            other = landed[0, plane, part, :] if odd else s_ref[1, plane, part, :]
            o_ref[0, plane, part, :] = jnp.where(chosen, landed[1, plane, part, :], other)

        by_rows(rows, 128, pick)
    for plane in copies:
        for copy in plane[:across]:
            copy.wait_recv()
    for plane in copies:
        for copy in plane:
            copy.wait_send()


def exchanged(row_key, odd, state, value):
    whole = pl.BlockSpec(memory_space=pltpu.VMEM)
    return pl.pallas_call(
        functools.partial(exchange, row_key, odd),
        out_shape=(state, value),
        in_specs=[whole] * 2,
        out_specs=[whole] * 2,
        scratch_shapes=[
            pltpu.VMEM(state.shape, jnp.float32),
            pltpu.VMEM((2, STAGE, 1, LANES), jnp.float32),
            pltpu.SemaphoreType.REGULAR,
            pltpu.SemaphoreType.REGULAR,
            pltpu.SemaphoreType.REGULAR,
            pltpu.SemaphoreType.DMA((2,)),
            pltpu.SemaphoreType.DMA((2,)),
            pltpu.SemaphoreType.DMA((2, 3)),
            pltpu.SemaphoreType.DMA((2, 2, 3)),
        ],
        compiler_params=pltpu.CompilerParams(
            collective_id=2 * row_key + odd, has_side_effects=True
        ),
        name="exchange",
    )


def gather(
    p_ref, m_ref, v_ref, g_hbm, old_hbm, new_hbm,
    s_ref, t_ref, key0_hbm, key1_hbm,
    g_ref, both, old_smem, new_smem, key_smem, sums, sems, state_sems, core_sems,
):
    row, col = lax.axis_index("row"), lax.axis_index("col")
    twin = (row, flip(col, 1))
    barrier = pltpu.get_barrier_semaphore()
    pl.semaphore_signal(barrier, inc=1, device_id=twin, device_id_type=MESH)
    smalls = [
        pltpu.make_async_copy(old_hbm.at[:, pl.ds(0, LANES)], old_smem, sems.at[0]),
        pltpu.make_async_copy(new_hbm.at[:, pl.ds(0, LANES)], new_smem, sems.at[1]),
    ]
    gradient = pltpu.make_async_copy(g_hbm, g_ref, sems.at[2])
    gradient.start()
    for copy in smalls:
        copy.start()
    copies = []
    for number, source in enumerate((p_ref, m_ref, v_ref)):
        copies.append(
            pltpu.make_async_copy(source, both.at[0, :, number], state_sems.at[0, number])
        )
        copies[-1].start()
    pl.semaphore_wait(barrier, 1)
    for number, source in enumerate((p_ref, m_ref, v_ref)):
        copies.append(
            pltpu.make_async_remote_copy(
                src_ref=source,
                dst_ref=both.at[1, :, number],
                send_sem=state_sems.at[1, number],
                recv_sem=state_sems.at[2, number],
                device_id=twin,
                device_id_type=MESH,
            )
        )
        copies[-1].start()
    gradient.wait()
    tensors, length, _ = g_ref.shape
    step = 64

    def body(i, total):
        at = pl.ds(pl.multiple_of(i * step, step), step)
        for tensor in range(tensors):
            g = g_ref[tensor, at, :].reshape(step // SUBLANES, SUBLANES, LANES)
            total = total + jnp.sum(g * g, axis=0)
        return total

    total = lax.fori_loop(0, length // step, body, jnp.zeros((SUBLANES, LANES), jnp.float32))
    sums[0] = jnp.sum(total, axis=0, keepdims=True)
    for copy in smalls:
        copy.wait()
    rows, odds, cores = [], [], []
    for tensor in range(2):
        old = old_smem[tensor, 0]
        route = jnp.bitwise_xor(jnp.right_shift(old, 1), new_smem[tensor, 0])
        key_y = jnp.bitwise_and(jnp.right_shift(route, 1), 3)
        odd = jnp.bitwise_and(key_y, 1)
        second = jnp.where(key_y >= 2, 1.0, 0.0)
        rows.append(jnp.right_shift(route, 3))
        odds.append(odd)
        cores.append(jnp.bitwise_and(route, 1))
        t_ref[3 - tensor] = jnp.full((1, LANES), second, jnp.float32)
        swapped = jnp.where(jnp.bitwise_and(old, 1) == 1, 1.0, 0.0)
        t_ref[4 + tensor] = jnp.full((1, LANES), swapped, jnp.float32)
    keys = []
    for turn, target in enumerate((key0_hbm, key1_hbm)):
        key_smem[turn, 0] = 2 * rows[turn] + odds[1 - turn]
        keys.append(pltpu.make_async_copy(key_smem.at[turn], target, sems.at[3 + turn]))
    swap = pltpu.make_async_remote_copy(
        src_ref=sums.at[0],
        dst_ref=sums.at[1],
        send_sem=core_sems.at[0],
        recv_sem=core_sems.at[1],
        device_id=twin,
        device_id_type=MESH,
    )
    swap.start()
    for number in range(3):
        for copy in copies[number::3]:
            copy.wait()
        if number == 0:
            for copy in keys:
                copy.start()

        def pick(part, number=number):
            for tensor in range(tensors):
                s_ref[tensor, number, part, :] = jnp.where(
                    cores[tensor] == 1,
                    both[1, tensor, number, part, :],
                    both[0, tensor, number, part, :],
                )

        by_rows(length, 64, pick)
    for copy in keys:
        copy.wait()
    swap.wait()
    t_ref[0] = sums[0] + sums[1]
    t_ref[1] = sums[0] + sums[1]


def adam_update(params, first_moment, second_moment, gradients, clip_factor):
    scaled = clip_factor * gradients
    first_new = beta_one * first_moment + (1.0 - beta_one) * scaled
    second_new = beta_two * second_moment + (1.0 - beta_two) * scaled * scaled
    bias_first = 1.0 - beta_one**STEP
    bias_second = 1.0 - beta_two**STEP
    update = first_new * (1.0 / bias_first) / (jnp.sqrt(second_new * (1.0 / bias_second)) + epsilon)
    params_new = params - learn_rate * (update + decay_rate * params)
    return (params_new, first_new, second_new)


def adam(limit, t_ref, s_ref, g_hbm, po_hbm, mo_hbm, vo_hbm, po_ref, mo_ref, vo_ref, g_ref, sems, loads):
    gradient = [
        pltpu.make_async_copy(g_hbm.at[tensor], g_ref.at[tensor], loads.at[tensor])
        for tensor in range(2)
    ]
    for copy in gradient:
        copy.start()
    squares = jnp.full((SUBLANES, LANES), jnp.sum(t_ref[1]), jnp.float32)
    clip = limit / jnp.maximum(jnp.sqrt(squares), limit)
    length = s_ref.shape[2]
    half = length // 2
    step = 64
    tile = (step // SUBLANES, SUBLANES, LANES)
    outputs = ((po_ref, po_hbm), (mo_ref, mo_hbm), (vo_ref, vo_hbm))
    for tensor in range(2):
        crossed = jnp.broadcast_to(t_ref[4 + tensor], (step, LANES)) > 0.5

        def lay(i, carry, crossed=crossed, tensor=tensor):
            for number, (ref, _) in enumerate(outputs):
                even, odd = (
                    s_ref[tensor, number, pl.ds(side + 2 * i * step, step, stride=2), :]
                    for side in range(2)
                )
                for side, value in enumerate(
                    (jnp.where(crossed, odd, even), jnp.where(crossed, even, odd))
                ):
                    at = pl.ds(pl.multiple_of(side * half + i * step, step), step)
                    ref[tensor, at, :] = value
            return carry

        lax.fori_loop(0, half // step, lay, 0)
    copies = []
    parts = 4
    step = length // parts
    tile = (step // SUBLANES, SUBLANES, LANES)
    for tensor in range(2):
        gradient[tensor].wait()

        def update(i, carry, tensor=tensor):
            at = pl.ds(pl.multiple_of(i * step, step), step)
            values = [ref[tensor, at, :].reshape(tile) for ref in (po_ref, mo_ref, vo_ref, g_ref)]
            for (ref, _), value in zip(outputs, adam_update(*values, clip[None])):
                ref[tensor, at, :] = value.reshape(step, LANES)
            return carry

        for part in range(parts):
            steps = length // step // parts
            lax.fori_loop(part * steps, (part + 1) * steps, update, 0)
            at = pl.ds(part * steps * step, steps * step)
            for number, (source, target) in enumerate(outputs):
                copy = pltpu.make_async_copy(
                    source.at[tensor, at], target.at[tensor, at], sems.at[tensor, part, number]
                )
                copy.start()
                copies.append(copy)
    for copy in copies:
        copy.wait()


def chosen_branch(index, branches, *operands):
    traced = jax.make_jaxpr(lambda i, *xs: lax.switch(i, branches, *xs))(index, *operands)
    choice = traced.eqns[-1]
    return choice.primitive.bind(index, *operands, **choice.params)


def shards(total, old_params, old_first, old_second, gradients, old_table, new_table):
    tensors, _, width = old_params.shape
    rows = 2 * width // LANES

    def lined(x):
        x = x.reshape(tensors, 2, width // LANES, LANES)
        return x.transpose(0, 2, 1, 3).reshape(tensors, rows, LANES)

    anywhere = pl.BlockSpec(memory_space=pl.ANY)
    whole = pl.BlockSpec(memory_space=pltpu.VMEM)
    state = jax.ShapeDtypeStruct((tensors, 3, rows, LANES), jnp.float32)
    value = jax.ShapeDtypeStruct((6, 1, LANES), jnp.float32)
    key = jax.ShapeDtypeStruct((1,), jnp.int32)
    full = jax.ShapeDtypeStruct((tensors, rows, LANES), jnp.float32)
    variants = [(row_key, odd) for row_key in range(16) for odd in range(2)]
    gradients = gradients.reshape(tensors, rows, LANES)
    stacked, shared, *keys = pl.pallas_call(
        gather,
        out_shape=(state, value, key, key),
        in_specs=[anywhere] * 6,
        out_specs=[whole] * 2 + [anywhere] * 2,
        scratch_shapes=[
            pltpu.VMEM(full.shape, jnp.float32),
            pltpu.VMEM((2, *state.shape), jnp.float32),
            pltpu.SMEM((tensors, LANES), jnp.int32),
            pltpu.SMEM((tensors, LANES), jnp.int32),
            pltpu.SMEM((2, 1), jnp.int32),
            pltpu.VMEM((2, 1, LANES), jnp.float32),
            pltpu.SemaphoreType.DMA((5,)),
            pltpu.SemaphoreType.DMA((3, 3)),
            pltpu.SemaphoreType.DMA((2,)),
        ],
        compiler_params=pltpu.CompilerParams(
            collective_id=len(variants), has_side_effects=True
        ),
        name="gather",
    )(
        *(lined(x) for x in (old_params, old_first, old_second)),
        gradients,
        old_table,
        new_table,
    )
    branches = [exchanged(row_key, odd, state, value) for row_key, odd in variants]

    for key in keys:
        stacked, shared = chosen_branch(key.reshape(()), branches, stacked, shared)
    new = pl.pallas_call(
        functools.partial(adam, 0.5 * math.sqrt(gradients.size * total)),
        out_shape=(full,) * 3,
        in_specs=[whole] * 2 + [anywhere],
        out_specs=[anywhere] * 3,
        scratch_shapes=[pltpu.VMEM(full.shape, jnp.float32)] * 4
        + [pltpu.SemaphoreType.DMA((tensors, 4, 3)), pltpu.SemaphoreType.DMA((tensors,))],
        name="adam",
    )(shared, stacked, gradients)
    return tuple(x.reshape(tensors, 1, rows * LANES) for x in new)


def solution(mesh):
    split = P(None, AXES, None)
    return jax.shard_map(
        functools.partial(shards, mesh.size),
        mesh=mesh,
        in_specs=(split,) * 4 + (P(), P()),
        out_specs=(split,) * 3,
        check_vma=False,
    )
```
